256 devices in a mesh: dp: 8 (over y, core), expert: 8 (over z), ffn: 4 (over x).
Axes of the slice: x: 4, y: 4, z: 8, core: 2. Of those that a mesh axis runs over, the one named last changes fastest.
Arguments:
- tokens: bfloat16 [512, 6144], P(('dp', 'expert'), 'ffn'), may hold values from -6 to 6
- out_grad: bfloat16 [512, 6144], P(('dp', 'expert'), 'ffn'), may hold values from -6 to 6
- expert_ids: int32 [512, 2], P(('dp', 'expert')), may hold values from 0 to 7, all different within a row; in each aligned block of 8 rows (0 to 7, 8 to 15, ...) at most 3 rows name the same one
- tenant_ids: int32 [512], P(('dp', 'expert')), may hold values from 0 to 7
- router_logits: float32 [512, 2], P(('dp', 'expert')), may hold values from -8 to 8
- gate_projection_weight: bfloat16 [8, 6144, 8192], P('expert', None, ('dp', 'ffn')), may hold values from -0.078125 to 0.078125
- up_projection_weight: bfloat16 [8, 6144, 8192], P('expert', None, ('dp', 'ffn')), may hold values from -0.078125 to 0.078125
- down_projection_weight: bfloat16 [8, 8192, 6144], P('expert', ('dp', 'ffn')), may hold values from -0.0625 to 0.0625
- input_down_maps: bfloat16 [8, 6144, 256], P('expert', 'ffn'), may hold values from -0.078125 to 0.078125
- input_up_maps: bfloat16 [8, 2, 128, 8192], P('expert', None, None, ('dp', 'ffn')), may hold values from -1.5 to 1.5
- output_down_map: bfloat16 [8, 8192, 128], P('expert', ('dp', 'ffn')), may hold values from -0.0625 to 0.0625
- output_up_map: bfloat16 [8, 128, 6144], P('expert', None, 'ffn'), may hold values from -1.5 to 1.5
Outputs:
- mixed: bfloat16 [512, 6144], P(('dp', 'expert'), 'ffn')
- input_grad: bfloat16 [512, 6144], P(('dp', 'expert'), 'ffn')
- input_down_gradient: float32 [8, 6144, 256], P('expert', 'ffn')
- input_up_gradient: float32 [8, 2, 128, 8192], P('expert', None, None, ('dp', 'ffn'))
- output_down_gradient: float32 [8, 8192, 128], P('expert', ('dp', 'ffn'))
- output_up_gradient: float32 [8, 128, 6144], P('expert', None, 'ffn')
The draws below stay inside these ranges and needn't reach their ends.
Inputs may be any that keep to these rules, and one draw needn't show every extreme that they name: `expert_ids`: each row names 2 different experts. Among the rows of one device's block of 8 tokens no expert is named more than 3 times; in some blocks one expert is named exactly 3 times.
All inputs are finite; a program needn't handle non-finite values.
Results may differ from the reference program's by a relative error of at most 0.0073.
Values may be sent and summed in bfloat16 or wider, within the bound.
No kernel may reach another device: no remote copies, remote signals or barrier semaphores. Data moves between devices by JAX's collectives and lax.ppermute only.
A program may use at most 256 MiB of HBM per device.

```python
import math
import jax
import jax.numpy as jnp
import numpy as np
from jax import lax

D = 6144
FF = 8192
RANK = 16
TENANTS = 8
TOP = 2
TOK_DEV = 8
EXPERTS = 8
TOKENS = 512
CAP = 3
ROWS = 192
TENANT_RANKS = 128


def touch_ends(drawn, stream_key, low, largest):
    place = [jax.random.randint(jax.random.fold_in(stream_key, axis), (), 0, length) for axis, length in enumerate(drawn.shape)]
    main_axis = drawn.shape.index(max(drawn.shape))
    next_to = place[:main_axis] + [(place[main_axis] + 1) % drawn.shape[main_axis]] + place[main_axis + 1:]
    return drawn.at[tuple(place)].set(low).at[tuple(next_to)].set(largest)


def block_levels(key, dims, split, least, high):
    factor_of = 1.0
    for dim, shards_of in split:
        heights = jax.random.uniform(jax.random.fold_in(jax.random.fold_in(key, 6), dim), (shards_of,), jnp.float32, least / len(split), high / len(split))
        factor_of = factor_of * jnp.repeat(jnp.exp(heights), dims[dim] // shards_of).reshape((-1,) + (1,) * (len(dims) - 1 - dim))
    return factor_of


def routed_block(stream_key, own, number, rows, number_of, top, limit, lean):
    order = jax.random.permutation(stream_key, number_of)
    heavy_load, ordinary = shares(number_of, rows * top, limit, lean, True), shares(number_of, rows * top, limit, lean, False)
    places = jnp.arange(number_of)

    def named(tallies, offset_by):
        used = int((tallies > 0).sum())
        fixed = max(1, used // 4)
        shifted = fixed + (places - fixed + offset_by * (used - fixed)) % max(1, number_of - fixed)
        return jnp.zeros((number_of,), jnp.int32).at[order[jnp.where(places < fixed, places, shifted)]].set(jnp.asarray(tallies, jnp.int32))

    tallies = jnp.where(number % 4 == 0, named(heavy_load, number // 4), named(ordinary, number - number // 4 - 1))
    mixed = jax.random.permutation(jax.random.fold_in(own, 3), number_of)
    source_of, sink = mixed[0:number_of // 2 * 2:2], mixed[1:number_of // 2 * 2:2]
    margin = jnp.minimum(tallies[source_of] - 1, limit - tallies[sink]) // 2
    margin = jnp.where((source_of == order[0]) | (sink == order[0]) | (tallies[sink] == 0), 0, jnp.maximum(margin, 0))
    shifted = jax.random.randint(jax.random.fold_in(own, 4), (number_of // 2,), 0, 1 << 20) % (margin + 1)
    tallies = tallies.at[source_of].add(-shifted).at[sink].add(shifted)
    members = jnp.searchsorted(jnp.cumsum(tallies), jnp.arange(rows * top), side="right").astype(jnp.int32)
    table = members.reshape(top, rows).T
    table = table[jax.random.permutation(jax.random.fold_in(own, 1), rows)]
    offset_by = jax.random.randint(jax.random.fold_in(own, 2), (rows, 1), 0, top)
    return jnp.take_along_axis(table, (jnp.arange(top)[None, :] + offset_by) % top, axis=1)


def shares(count, total, most, skew, full):
    weights = [(1 << 20) // math.isqrt(grade ** skew) + 1 for grade in range(1, count + 1)]
    largest = most if full else min(most, max(-(-total // count), total * weights[0] // sum(weights)))
    least = 1 if total - largest >= count - 1 else 0
    given, rest = [largest] + [least] * (count - 1), total - largest - least * (count - 1)
    while rest > 0:
        candidates = [i for i in range(1, count) if given[i] < largest] or [i for i in range(1, count) if given[i] < most]
        mass, remaining = sum([weights[i] for i in candidates]), rest
        for i in candidates:
            extra = min(most - given[i], max(1, remaining * weights[i] // mass), rest)
            given[i] = given[i] + extra
            rest = rest - extra
    return np.array(given)


def scatter_about(own_key, dims, deviation, reach, shards=(), kind=jnp.bfloat16):
    entries = deviation * jax.random.normal(own_key, dims, jnp.float32)
    if shards:
        entries = entries * block_levels(own_key, dims, shards, -0.22, 0.18)
    return jnp.clip(entries, -reach, reach).astype(kind)


def setup_inputs(seed: int = 0) -> dict:
    keys = jax.random.split(jax.random.key(seed), 13)
    tokens = scatter_about(keys[0], (TOKENS, D), 1.0, 6.0, ((0, 64), (1, 4)))
    out_grad = scatter_about(keys[1], (TOKENS, D), 1.0, 6.0, ((0, 64), (1, 4)))
    expert_ids_keys = jax.random.split(jax.random.fold_in(keys[2], 1), TOKENS // TOK_DEV)
    expert_ids_turns = jax.random.permutation(jax.random.fold_in(keys[2], 3), TOKENS // TOK_DEV)
    expert_ids = jax.vmap(lambda own, number: routed_block(jax.random.fold_in(keys[2], 2), own, number, TOK_DEV, EXPERTS, TOP, CAP, 2))(expert_ids_keys, expert_ids_turns).reshape((TOKENS, TOP))
    tenant_ids = touch_ends(jax.random.randint(keys[3], (TOKENS,), 0, TENANTS), jax.random.fold_in(keys[3], 1), 0, TENANTS - 1).astype(jnp.int32)
    router_logits = scatter_about(keys[4], (TOKENS, TOP), 1.5, 8.0, ((0, 64),), jnp.float32)
    gate_projection_weight = scatter_about(keys[5], (EXPERTS, D, FF), D ** -0.5, 0.078125, ((0, 8), (2, 32)))
    up_projection_weight = scatter_about(keys[6], (EXPERTS, D, FF), D ** -0.5, 0.078125, ((0, 8), (2, 32)))
    down_projection_weight = scatter_about(keys[7], (EXPERTS, FF, D), FF ** -0.5, 0.0625, ((0, 8), (1, 32)))
    input_down_maps = scatter_about(keys[8], (EXPERTS, D, 2 * TENANT_RANKS), D ** -0.5, 0.078125, ((0, 8), (1, 4)))
    input_up_maps = scatter_about(keys[9], (EXPERTS, 2, TENANT_RANKS, FF), RANK ** -0.5, 1.5, ((0, 8), (3, 32)))
    output_down_map = scatter_about(keys[10], (EXPERTS, FF, TENANT_RANKS), FF ** -0.5, 0.0625, ((0, 8), (1, 32)))
    output_up_map = scatter_about(keys[11], (EXPERTS, TENANT_RANKS, D), RANK ** -0.5, 1.5, ((0, 8), (2, 4)))
    return {"tokens": tokens, "out_grad": out_grad, "expert_ids": expert_ids, "tenant_ids": tenant_ids, "router_logits": router_logits, "gate_projection_weight": gate_projection_weight, "up_projection_weight": up_projection_weight, "down_projection_weight": down_projection_weight, "input_down_maps": input_down_maps, "input_up_maps": input_up_maps, "output_down_map": output_down_map, "output_up_map": output_up_map}


ADAPTER_SCALE = 0.5


def matrix_product(left, right):
    return jnp.dot(left, right, preferred_element_type=jnp.float32)


def slot_rows(expert_ids):
    blocked = expert_ids.reshape(-1, TOK_DEV * TOP)
    labels = jnp.arange(EXPERTS, dtype=jnp.int32)
    onehot = (blocked[:, :, None] == labels[None, None, :]).astype(jnp.int32)
    before = jnp.cumsum(onehot, axis=1) - onehot
    position = jnp.sum(before * onehot, axis=2).astype(jnp.int32)
    block_index = jnp.arange(blocked.shape[0], dtype=jnp.int32)[:, None]
    return (block_index * CAP + position).reshape(-1, TOP).astype(jnp.int32)


def expert_step(inputs):
    (expert_token_rows, expert_gradients, exp_tenant, gate_matrix, up_matrix, down_matrix,
     expert_input_down, expert_input_up, expert_output_down, expert_output_up) = inputs
    columns = jnp.arange(TENANT_RANKS, dtype=jnp.int32) // RANK
    tenant_column_mask = (exp_tenant[:, None] == columns[None, :]).astype(jnp.float32)
    paired_mask = jnp.concatenate([tenant_column_mask, tenant_column_mask], axis=1)
    adapter_input = matrix_product(expert_token_rows, expert_input_down)
    adapter_rows = (paired_mask * adapter_input).astype(jnp.bfloat16)
    gate_activation = matrix_product(expert_token_rows, gate_matrix) + ADAPTER_SCALE * matrix_product(adapter_rows[:, :TENANT_RANKS], expert_input_up[0])
    up_activation = matrix_product(expert_token_rows, up_matrix) + ADAPTER_SCALE * matrix_product(adapter_rows[:, TENANT_RANKS:], expert_input_up[1])
    activated = jax.nn.silu(gate_activation)
    hidden_state = (activated * up_activation).astype(jnp.bfloat16)
    down_adapter_term = matrix_product(hidden_state, expert_output_down)
    down_row_values = (tenant_column_mask * down_adapter_term).astype(jnp.bfloat16)
    expert_output = (matrix_product(hidden_state, down_matrix) + ADAPTER_SCALE * matrix_product(down_row_values, expert_output_up)).astype(jnp.bfloat16)
    adapter_backward = matrix_product(expert_gradients, expert_output_up.T)
    backward_rows = (tenant_column_mask * adapter_backward).astype(jnp.bfloat16)
    hidden_gradient = matrix_product(expert_gradients, down_matrix.T) + ADAPTER_SCALE * matrix_product(backward_rows, expert_output_down.T)
    output_down_gradient = ADAPTER_SCALE * matrix_product(hidden_state.T, backward_rows)
    output_up_gradient = ADAPTER_SCALE * matrix_product(down_row_values.T, expert_gradients)
    sigmoid_gate = jax.nn.sigmoid(gate_activation)
    gate_gradient = (hidden_gradient * up_activation * sigmoid_gate * (1.0 + gate_activation * (1.0 - sigmoid_gate))).astype(jnp.bfloat16)
    up_gradient = (hidden_gradient * activated).astype(jnp.bfloat16)
    input_up_gradient = ADAPTER_SCALE * jnp.stack([matrix_product(adapter_rows[:, :TENANT_RANKS].T, gate_gradient), matrix_product(adapter_rows[:, TENANT_RANKS:].T, up_gradient)])
    up_adapter_term = jnp.concatenate([matrix_product(gate_gradient, expert_input_up[0].T), matrix_product(up_gradient, expert_input_up[1].T)], axis=1)
    up_row_values = (paired_mask * up_adapter_term).astype(jnp.bfloat16)
    input_down_gradient = ADAPTER_SCALE * matrix_product(expert_token_rows.T, up_row_values)
    running_partial_sum = matrix_product(gate_gradient, gate_matrix.T) + matrix_product(up_gradient, up_matrix.T)
    input_result = (running_partial_sum + ADAPTER_SCALE * matrix_product(up_row_values, expert_input_down.T)).astype(jnp.bfloat16)
    return expert_output, input_result, input_down_gradient, input_up_gradient, output_down_gradient, output_up_gradient


def reference(tokens, out_grad, expert_ids, tenant_ids, router_logits, gate_projection_weight, up_projection_weight, down_projection_weight, input_down_maps, input_up_maps, output_down_map, output_up_map):
    slot_index = slot_rows(expert_ids)
    flat_index = (expert_ids * ROWS + slot_index).reshape(-1).astype(jnp.int32)
    prob_first = jax.nn.sigmoid(router_logits[:, 0] - router_logits[:, 1])
    gate_probs = jnp.stack([prob_first, 1.0 - prob_first], axis=1)
    total_rows = EXPERTS * ROWS
    token_copies = jnp.repeat(tokens, TOP, axis=0)
    grad_copies = (gate_probs[:, :, None] * out_grad.astype(jnp.float32)[:, None, :]).astype(jnp.bfloat16).reshape(-1, D)
    tenant_copies = jnp.repeat(tenant_ids, TOP).astype(jnp.int32)
    expert_token_rows = jnp.zeros((total_rows, D), jnp.bfloat16).at[flat_index].set(token_copies)
    expert_gradients = jnp.zeros((total_rows, D), jnp.bfloat16).at[flat_index].set(grad_copies)
    exp_tenant = jnp.full((total_rows,), -1, jnp.int32).at[flat_index].set(tenant_copies)
    results = lax.map(expert_step, (expert_token_rows.reshape(EXPERTS, ROWS, D), expert_gradients.reshape(EXPERTS, ROWS, D),
                                    exp_tenant.reshape(EXPERTS, ROWS), gate_projection_weight, up_projection_weight, down_projection_weight, input_down_maps, input_up_maps, output_down_map, output_up_map))
    expert_output, input_result, input_down_gradient, input_up_gradient, output_down_gradient, output_up_gradient = results
    out_picked = expert_output.reshape(total_rows, D).astype(jnp.float32)[flat_index].reshape(-1, TOP, D)
    mixed = jnp.sum(gate_probs[:, :, None] * out_picked, axis=1).astype(jnp.bfloat16)
    grad_picked = input_result.reshape(total_rows, D).astype(jnp.float32)[flat_index].reshape(-1, TOP, D)
    input_grad = jnp.sum(grad_picked, axis=1).astype(jnp.bfloat16)
    return mixed, input_grad, input_down_gradient, input_up_gradient, output_down_gradient, output_up_gradient
```

```python
import jax
import jax.numpy as jnp
from jax import lax
from jax.experimental import pallas as pl
from jax.experimental.pallas import tpu as pltpu
from jax.sharding import PartitionSpec as P

RANK = 16
SCALE = 0.5
SLOTS = 3
GROUP = 8
LANES = 128
BF = jnp.bfloat16
F32 = jnp.float32
I32 = jnp.int32


def dot(left, right, dims=((1,), (0,))):
    return lax.dot_general(left, right, (dims, ((), ())), preferred_element_type=F32)


def rows_of(shape):
    return lax.broadcasted_iota(I32, shape, 0)


def lanes_of(shape):
    return lax.broadcasted_iota(I32, shape, 1)


def onehot(condition):
    return jnp.where(condition, 1.0, 0.0).astype(BF)


def two_parts(value):
    high = value.astype(BF)
    return high, (value - high.astype(F32)).astype(BF)


def vmem():
    return pl.BlockSpec(memory_space=pltpu.VMEM)


def smem():
    return pl.BlockSpec(memory_space=pltpu.SMEM)


def anywhere():
    return pl.BlockSpec(memory_space=pl.ANY)


def place_of(where):
    return where[0], where[1], where[2]


def codes_of(ids):
    n_rows, n_top = ids.shape
    chosen = [ids[t, k] for t in range(n_rows) for k in range(n_top)]
    codes = []
    for i, expert in enumerate(chosen):
        position = jnp.int32(0)
        for earlier in chosen[:i]:
            position += jnp.where(earlier == expert, 1, 0).astype(I32)
        codes.append((i // n_top, i % n_top, expert, position))
    return codes


def gates(logits):
    first = jax.nn.sigmoid(logits[:, 0:1] - logits[:, 1:2])
    return first, 1.0 - first


def dispatch_kernel(ids, tenants, logits, tokens, grads, out):
    n_out = out.shape[0]
    n_rows = tokens.shape[0]
    codes = codes_of(ids)
    first, second = gates(logits[...])
    row = rows_of((n_out, LANES))
    lane = lanes_of((n_out, LANES))
    pick_token = jnp.zeros((n_out, LANES), F32)
    pick_grad = jnp.zeros((n_out, LANES), F32)
    tenant_row = jnp.zeros((n_out, LANES), F32)
    for t, k, expert, position in codes:
        base = expert * GROUP
        pick_token = jnp.where((row == base + position) & (lane == t), 1.0, pick_token)
        pick_grad = jnp.where(
            (row == base + SLOTS + position) & (lane == t + k * n_rows), 1.0, pick_grad
        )
        code = (tenants[t] + 1).astype(F32)
        tenant_row = jnp.where(
            (row == base + 2 * SLOTS) & (lane == position), code, tenant_row
        )
    g = grads[...].astype(F32)
    scaled = jnp.concatenate([(first * g).astype(BF), (second * g).astype(BF)], axis=0)
    value = dot(pick_token[:, :n_rows].astype(BF), tokens[...]) + dot(
        pick_grad[:, : 2 * n_rows].astype(BF), scaled
    )
    out[...] = value.astype(BF)
    out[:, :LANES] = (value[:, :LANES] + tenant_row).astype(BF)


def received_kernel(where, arrived, down_maps, up_map, keep, send):
    n_in, width = arrived.shape
    n = keep.shape[0]
    core = where[2]
    row = rows_of((n, n_in))
    column = lanes_of((n, n_in))
    start = (row // SLOTS) * GROUP
    offset = row % SLOTS
    data = arrived[...]
    tokens = dot(onehot(column == start + offset), data).astype(BF)
    grads = dot(onehot(column == start + SLOTS + offset), data).astype(BF)
    tenants = dot(onehot(column == start + 2 * SLOTS), data[:, :LANES])
    lane = lanes_of((n, LANES))
    tenant = jnp.sum(
        jnp.where(lane == rows_of((n, LANES)) % SLOTS, tenants, 0.0), axis=1, keepdims=True
    )
    mask = jnp.where((lane // RANK + 1).astype(F32) == tenant, 1.0, 0.0)
    product = dot(tokens, down_maps[0])
    back = dot(grads, up_map[0], ((1,), (1,)))
    source = rows_of((LANES, LANES)) % RANK
    target = lanes_of((LANES, LANES))

    def moved(value, offset):
        return dot(value, onehot(target - offset == source))

    gate_high, gate_low = two_parts(mask * product[:, :LANES])
    up_high, up_low = two_parts(mask * product[:, LANES:])
    back_high, back_low = two_parts(mask * back)
    token_extra = (
        moved(gate_high, 0)
        + moved(up_high, RANK)
        + moved(gate_low, 2 * RANK)
        + moved(up_low, 3 * RANK)
        + jnp.where(lane == 4 * RANK, tenant, 0.0)
    ).astype(BF)
    grad_extra = (moved(back_high, 0) + moved(back_low, RANK)).astype(BF)

    @pl.when(core == 0)
    def _():
        keep[:, :width] = tokens
        keep[:, width:] = token_extra
        send[:, :width] = grads
        send[:, width:] = grad_extra

    @pl.when(core != 0)
    def _():
        keep[:, :width] = grads
        keep[:, width:] = grad_extra
        send[:, :width] = tokens
        send[:, width:] = token_extra


def expert_kernel(
    where,
    own0, own1, own2, own3,
    far0, far1, far2, far3,
    gate_w, up_w, down_w, up_maps, out_down,
    keep0, keep1, keep2, keep3,
    send0, send1, send2, send3,
    token_part, grad_part,
    input_up_grad, output_down_grad,
    x_v, g_v, wg_v, wu_v, wd_v, y_v, d_v,
    sem_x, sem_g, sem_wg, sem_wu, sem_wd, sem_y, sem_d, sem_t,
):
    own = (own0, own1, own2, own3)
    far = (far0, far1, far2, far3)
    keep = (keep0, keep1, keep2, keep3)
    send = (send0, send1, send2, send3)
    n = len(own)
    rows = own0.shape[1]
    width = wg_v.shape[1]
    x, y, core = place_of(where)
    copy = pltpu.make_async_copy
    span = lambda t: pl.ds(t * rows, rows)

    def fetch(tokens, grads):
        for s in range(n):
            for t in range(n):
                copy(tokens[t].at[s], x_v.at[s, span(t)], sem_x.at[s]).start()
        for s in range(n):
            for t in range(n):
                copy(grads[s].at[t], g_v.at[s, span(t)], sem_g.at[s]).start()

    def weights(s):
        start = pl.multiple_of(((x - s + n) % n) * width, width)
        return (
            copy(gate_w.at[0, pl.ds(start, width), :], wg_v.at[s], sem_wg.at[s]),
            copy(up_w.at[0, pl.ds(start, width), :], wu_v.at[s], sem_wu.at[s]),
            copy(down_w.at[0, :, pl.ds(start, width)], wd_v.at[s], sem_wd.at[s]),
        )

    @pl.when(core == 0)
    def _():
        fetch(own, far)

    @pl.when(core != 0)
    def _():
        fetch(far, own)

    copies = [weights(s) for s in range(n)]
    for s in range(n):
        copies[s][0].start()
        copies[s][1].start()
    for s in range(n):
        copies[s][2].start()

    def arrived(buffer, sem, s):
        copy(buffer.at[s], buffer.at[s], sem.at[s]).wait()

    total = n * rows
    gate = jnp.zeros((total, wg_v.shape[2]), F32)
    up = jnp.zeros((total, wg_v.shape[2]), F32)
    extra = jnp.zeros((total, LANES), F32)
    for s in range(n):
        arrived(x_v, sem_x, s)
        copies[s][0].wait()
        copies[s][1].wait()
        value = x_v[s, :, :width]
        gate += dot(value, wg_v[s])
        up += dot(value, wu_v[s])
        extra += x_v[s, :, width:].astype(F32)
    lane = lanes_of((total, LANES))
    tenant = jnp.sum(
        jnp.where(lane == 4 * RANK, x_v[0, :, width:].astype(F32), 0.0), axis=1, keepdims=True
    )
    mask = jnp.where((lane // RANK + 1).astype(F32) == tenant, 1.0, 0.0)

    for t in range(n):
        place = (y - t + n) % n
        copy(x_v.at[0, span(t)], token_part.at[place], sem_t.at[0]).start()

    row1 = rows_of((LANES, LANES))
    lane1 = lanes_of((LANES, LANES))
    spread = [onehot(row1 == lane1 % RANK + k * RANK) for k in range(2)]
    whole = (extra + pltpu.roll(extra, LANES - 2 * RANK, 1)).astype(BF)
    gate_rows = (mask * dot(whole, spread[0])).astype(BF)
    up_rows = (mask * dot(whole, spread[1])).astype(BF)
    gate += SCALE * dot(gate_rows, up_maps[0, 0])
    up += SCALE * dot(up_rows, up_maps[0, 1])
    sigmoid = jax.nn.sigmoid(gate)
    activated = gate * sigmoid
    hidden = (activated * up).astype(BF)
    down_part = mask * dot(hidden, out_down[0])

    for s in range(n):
        copies[s][2].wait()
        result = dot(hidden, wd_v[s]).astype(BF)
        for t in range(n):
            y_v[t, s, :, :width] = result[t * rows : (t + 1) * rows]

    grad_hidden = jnp.zeros((total, wg_v.shape[2]), F32)
    extra = jnp.zeros((total, LANES), F32)
    for s in range(n):
        arrived(g_v, sem_g, s)
        grad_hidden += dot(g_v[s, :, :width], wd_v[s], ((1,), (1,)))
        extra += g_v[s, :, width:].astype(F32)
    for t in range(n):
        place = (y - t + n) % n
        copy(g_v.at[0, span(t)], grad_part.at[place], sem_t.at[1]).start()
    whole = (extra + pltpu.roll(extra, LANES - RANK, 1)).astype(BF)
    back_rows = (mask * dot(whole, spread[0])).astype(BF)
    grad_hidden += SCALE * dot(back_rows, out_down[0], ((1,), (1,)))
    output_down_grad[0] = SCALE * dot(hidden, back_rows, ((0,), (0,)))
    grad_gate = (grad_hidden * up * sigmoid * (1.0 + gate * (1.0 - sigmoid))).astype(BF)
    grad_up = (grad_hidden * activated).astype(BF)
    input_up_grad[0, 0] = SCALE * dot(gate_rows, grad_gate, ((0,), (0,)))
    input_up_grad[0, 1] = SCALE * dot(up_rows, grad_up, ((0,), (0,)))
    gate_part = mask * dot(grad_gate, up_maps[0, 0], ((1,), (1,)))
    up_part = mask * dot(grad_up, up_maps[0, 1], ((1,), (1,)))

    def moved(value, offset):
        return dot(value, onehot(lane1 - offset == row1 % RANK))

    pieces = [two_parts(v) for v in (down_part, gate_part, up_part)]
    sums = jnp.zeros((total, LANES), F32)
    for k, (high, low) in enumerate(pieces):
        sums += moved(high, k * RANK) + moved(low, (k + 3) * RANK)
    sums = sums.astype(BF)
    for t in range(n):
        place = (y - t + n) % n
        block = sums[t * rows : (t + 1) * rows]
        for j in range(n):
            y_v[j, place, :, width:] = block
            d_v[j, place, :, width:] = block

    def put(buffer, out, sem):
        for j in range(n):
            copy(buffer.at[j], out[j], sem.at[j]).start()

    @pl.when(core == 0)
    def _():
        put(y_v, keep, sem_y)

    @pl.when(core != 0)
    def _():
        put(y_v, send, sem_y)

    for s in range(n):
        result = (
            dot(grad_gate, wg_v[s], ((1,), (1,))) + dot(grad_up, wu_v[s], ((1,), (1,)))
        ).astype(BF)
        for t in range(n):
            d_v[s, t, :, :width] = result[t * rows : (t + 1) * rows]

    @pl.when(core == 0)
    def _():
        put(d_v, send, sem_d)

    @pl.when(core != 0)
    def _():
        put(d_v, keep, sem_d)

    for j in range(n):
        copy(y_v.at[j], keep[j], sem_y.at[j]).wait()
        copy(d_v.at[j], send[j], sem_d.at[j]).wait()
    for t in range(n):
        copy(x_v.at[0, span(t)], token_part.at[t], sem_t.at[0]).wait()
        copy(g_v.at[0, span(t)], grad_part.at[t], sem_t.at[1]).wait()


def joined_extra(pieces):
    value = sum(p.astype(F32) for p in pieces)
    lane = lanes_of(value.shape)
    width = 3 * RANK
    whole = value + pltpu.roll(value, LANES - width, 1)
    whole = jnp.where(lane < width, whole, 0.0)
    high, low = two_parts(whole)
    return (high.astype(F32) + pltpu.roll(low.astype(F32), width, 1)).astype(BF)


def pair_kernel(mine, theirs, out):
    width = out.shape[2] - LANES
    a, b = mine[0], theirs[0]
    out[0, :, :width] = (a[:, :width].astype(F32) + b[:, :width].astype(F32)).astype(BF)
    out[0, :, width:] = joined_extra([a[:, width:], b[:, width:]])


def first_kernel(mine, theirs, near1, near2, near3, out0, out1, out2, out3):
    outs = (out0, out1, out2, out3)
    n = len(outs)
    width = mine.shape[2] - LANES
    arrays = (mine, theirs, near1, near2, near3)
    for i in range(n):
        outs[i][:, :width] = sum(a[i, :, :width].astype(F32) for a in arrays).astype(BF)
        extra = joined_extra([a[i, :, width:] for a in arrays])
        for out in outs:
            out[:, width + i * LANES : width + (i + 1) * LANES] = extra


def tenants_of(part, width):
    extra = part[:, width:].astype(F32)
    lane = lanes_of(extra.shape)
    tenant = jnp.sum(jnp.where(lane == 4 * RANK, extra, 0.0), axis=1, keepdims=True)
    return jnp.where((lane // RANK + 1).astype(F32) == tenant, 1.0, 0.0)


def last_kernel(
    where, mine, near1, near2, near3, token_part, down_maps, up_map,
    keep, send, down_rows, up_rows,
):
    arrays = (mine, near1, near2, near3)
    n = len(arrays)
    rows, width = mine.shape[0], keep.shape[1]
    half = rows // 2
    x, y, core = place_of(where)
    row1 = rows_of((LANES, LANES))
    lane1 = lanes_of((LANES, LANES))
    spread = [onehot(row1 == lane1 % RANK + k * RANK) for k in range(3)]
    for i in range(n):
        at = width + i * LANES
        value = sum(a[:, at : at + LANES].astype(F32) for a in arrays)
        whole = (value + pltpu.roll(value, LANES - 3 * RANK, 1)).astype(BF)
        mask = tenants_of(token_part[i], width)
        down_rows[i] = (mask * dot(whole, spread[0])).astype(BF)
        up_rows[i, :, :LANES] = (mask * dot(whole, spread[1])).astype(BF)
        up_rows[i, :, LANES:] = (mask * dot(whole, spread[2])).astype(BF)
    value = sum(a[:, :width].astype(F32) for a in arrays)

    @pl.when(core == 0)
    def _():
        result = (value + SCALE * dot(down_rows[y], up_map[0])).astype(BF)
        keep[...] = result[:half]
        send[...] = result[half:]

    @pl.when(core != 0)
    def _():
        result = (value + SCALE * dot(up_rows[y], down_maps[0], ((1,), (1,)))).astype(BF)
        keep[...] = result[half:]
        send[...] = result[:half]


def adapter_grad_kernel(token_part, grad_part, down_rows, up_rows, input_down_grad, output_up_grad):
    n, rows, _ = token_part.shape
    width = output_up_grad.shape[2]
    join = lambda ref, columns: jnp.concatenate([ref[i, :, :columns] for i in range(n)], axis=0)
    down = join(down_rows, LANES)
    up = join(up_rows, 2 * LANES)
    output_up_grad[0] = SCALE * dot(down, join(grad_part, width), ((0,), (0,)))
    input_down_grad[0] = SCALE * dot(join(token_part, width), up, ((0,), (0,)))


def return_kernel(mine, theirs, out):
    n_out, n = out.shape[0], mine.shape[0]
    row = rows_of((n_out, n))
    column = lanes_of((n_out, n))
    slot = row % GROUP
    base = (row // GROUP) * SLOTS
    first = onehot((slot < SLOTS) & (column == base + slot))
    second = onehot(
        (slot >= SLOTS) & (slot < 2 * SLOTS) & (column == base + slot - SLOTS)
    )
    out[...] = (dot(first, mine[...]) + dot(second, theirs[...])).astype(BF)


def combine_kernel(where, ids, logits, arrived, mixed, input_grad):
    n_in = arrived.shape[0]
    n_rows = mixed.shape[0]
    core = where[2]
    shift = core * SLOTS
    first, second = gates(logits[...])
    row = rows_of((n_rows, n_in))
    lane = lanes_of((n_rows, n_in))
    zero = jnp.zeros((n_rows, n_in), F32)
    picks = [[zero, zero], [zero, zero]]
    for t, k, expert, position in codes_of(ids):
        base = expert * GROUP + position
        picks[0][k] = jnp.where((row == t) & (lane == base + shift), 1.0, picks[0][k])
        picks[1][k] = jnp.where(
            (row == t) & (lane == base + SLOTS - shift), 1.0, picks[1][k]
        )
    data = arrived[...]
    value = [[dot(p.astype(BF), data) for p in pair] for pair in picks]
    mixed[...] = (first * value[0][0] + second * value[0][1]).astype(BF)
    input_grad[...] = (value[1][0] + value[1][1]).astype(BF)


def shape(dims, dtype=BF):
    return jax.ShapeDtypeStruct(tuple(dims), dtype)


def per_device(
    tokens,
    out_grad,
    expert_ids,
    tenant_ids,
    router_logits,
    gate_projection_weight,
    up_projection_weight,
    down_projection_weight,
    input_down_maps,
    input_up_maps,
    output_down_map,
    output_up_map,
):
    n_experts = lax.axis_size("expert")
    n_data = lax.axis_size("dp")
    n = lax.axis_size("ffn")
    n_rows, width = tokens.shape
    hidden = gate_projection_weight.shape[2]
    columns = output_down_map.shape[2]
    slots = SLOTS * n_experts
    pair = 2 * slots
    wide = width + LANES
    plane = ("dp", "ffn")
    data_index = lax.axis_index("dp")
    where = jnp.stack([lax.axis_index("ffn"), data_index // 2, data_index % 2]).astype(I32)

    def turn(distance, stage):
        pairs = []
        for chip in range(n):
            for core in range(2):
                for split in range(n):
                    if core == stage:
                        to = (chip, (split + distance) % n)
                    else:
                        to = ((chip + distance) % n, split)
                    pairs.append(
                        ((2 * chip + core) * n + split, (2 * to[0] + core) * n + to[1])
                    )
        return pairs

    def turned(value, distance, stage):
        return lax.ppermute(value, plane, turn(distance, stage))

    def swapped(value):
        return lax.ppermute(value, "dp", [(i, i ^ 1) for i in range(n_data)])

    def call(kernel, out, ins, **rest):
        return pl.pallas_call(
            kernel,
            out_shape=out,
            in_specs=ins,
            compiler_params=pltpu.CompilerParams(vmem_limit_bytes=56 * 1024 * 1024),
            **rest,
        )

    sent = call(
        dispatch_kernel,
        shape((n_experts * GROUP, width)),
        [smem(), smem(), vmem(), vmem(), vmem()],
        out_specs=vmem(),
    )(expert_ids, tenant_ids, router_logits, tokens, out_grad)
    arrived = lax.all_to_all(
        sent.reshape(n_experts, GROUP, width), "expert", 0, 0, tiled=True
    ).reshape(n_experts * GROUP, width)
    keep, send = call(
        received_kernel,
        [shape((slots, wide)), shape((slots, wide))],
        [smem(), vmem(), vmem(), vmem()],
        out_specs=[vmem(), vmem()],
    )(where, arrived, input_down_maps, output_up_map)
    other = swapped(send)
    first_core = where[2] == 0
    unit = jnp.concatenate(
        [jnp.where(first_core, keep, other), jnp.where(first_core, other, keep)], axis=0
    )
    line = [unit] + [turned(unit, s, 0) for s in range(1, n)]
    line = jnp.stack(line)
    own = [line] + [turned(line, s, 1) for s in range(1, n)]
    far = [swapped(v) for v in own]

    block = shape((n, pair, wide))
    part = shape((n, pair, wide))
    dma = pltpu.SemaphoreType.DMA
    results = call(
        expert_kernel,
        [block] * (2 * n)
        + [part, part, shape((1, 2, columns, hidden), F32), shape((1, hidden, columns), F32)],
        [smem()] + [anywhere()] * (2 * n + 3) + [vmem(), vmem()],
        out_specs=[anywhere()] * (2 * n + 2) + [vmem(), vmem()],
        scratch_shapes=[
            pltpu.VMEM((n, n * pair, wide), BF),
            pltpu.VMEM((n, n * pair, wide), BF),
            pltpu.VMEM((n, width, hidden), BF),
            pltpu.VMEM((n, width, hidden), BF),
            pltpu.VMEM((n, hidden, width), BF),
            pltpu.VMEM((n, n, pair, wide), BF),
            pltpu.VMEM((n, n, pair, wide), BF),
        ]
        + [dma((n,))] * 7
        + [dma((2,))],
    )(
        where,
        *own,
        *far,
        gate_projection_weight,
        up_projection_weight,
        down_projection_weight,
        input_up_maps,
        output_down_map,
    )
    keeps, sends = results[:n], results[n : 2 * n]
    token_part, grad_part, input_up_gradient, output_down_gradient = results[2 * n :]

    def summed(mine, theirs):
        spec = pl.BlockSpec((1, pair, wide), lambda i: (i, 0, 0))
        return pl.pallas_call(
            pair_kernel, out_shape=block, grid=(n,), in_specs=[spec, spec], out_specs=spec
        )(mine, theirs)

    theirs = {j: swapped(sends[j]) for j in (1, 2, 3, 0)}
    near = [turned(summed(keeps[j], theirs[j]), n - j, 1) for j in range(1, n)]
    tail = shape((pair, width + n * LANES))
    lines = call(
        first_kernel, [tail] * n, [vmem()] * (n + 1), out_specs=[vmem()] * n
    )(keeps[0], theirs[0], *near)
    near = [turned(lines[j], n - j, 0) for j in range(1, n)]
    keep, send, down_rows, up_rows = call(
        last_kernel,
        [
            shape((slots, width)),
            shape((slots, width)),
            shape((n, pair, columns)),
            shape((n, pair, 2 * columns)),
        ],
        [smem()] + [vmem()] * (n + 3),
        out_specs=[vmem()] * 4,
    )(where, lines[0], *near, token_part, input_down_maps, output_up_map)
    other = swapped(send)
    back = call(
        return_kernel, shape((n_experts * GROUP, width)), [vmem(), vmem()], out_specs=vmem()
    )(keep, other)
    back = lax.all_to_all(
        back.reshape(n_experts, GROUP, width), "expert", 0, 0, tiled=True
    ).reshape(n_experts * GROUP, width)
    input_down_gradient, output_up_gradient = call(
        adapter_grad_kernel,
        [shape((1, width, 2 * columns), F32), shape((1, columns, width), F32)],
        [vmem()] * 4,
        out_specs=[vmem(), vmem()],
    )(token_part, grad_part, down_rows, up_rows)
    mixed, input_grad = call(
        combine_kernel,
        [shape((n_rows, width)), shape((n_rows, width))],
        [smem(), smem(), vmem(), vmem()],
        out_specs=[vmem(), vmem()],
    )(where, expert_ids, router_logits, back)
    return (
        mixed,
        input_grad,
        input_down_gradient,
        input_up_gradient,
        output_down_gradient,
        output_up_gradient,
    )


def solution(mesh):
    return jax.shard_map(
        per_device,
        mesh=mesh,
        in_specs=(
            P(("dp", "expert"), "ffn"),
            P(("dp", "expert"), "ffn"),
            P(("dp", "expert"), None),
            P(("dp", "expert")),
            P(("dp", "expert"), None),
            P("expert", None, ("dp", "ffn")),
            P("expert", None, ("dp", "ffn")),
            P("expert", ("dp", "ffn"), None),
            P("expert", "ffn", None),
            P("expert", None, None, ("dp", "ffn")),
            P("expert", ("dp", "ffn"), None),
            P("expert", None, "ffn"),
        ),
        out_specs=(
            P(("dp", "expert"), "ffn"),
            P(("dp", "expert"), "ffn"),
            P("expert", "ffn", None),
            P("expert", None, None, ("dp", "ffn")),
            P("expert", ("dp", "ffn"), None),
            P("expert", None, "ffn"),
        ),
        check_vma=False,
    )
```

```python
import jax
import jax.numpy as jnp
from jax import lax
from jax.experimental import pallas as pl
from jax.experimental.pallas import tpu as pltpu
from jax.sharding import PartitionSpec as P

RANK = 16
SCALE = 0.5
SLOTS = 3
GROUP = 8
LANES = 128
BF = jnp.bfloat16
F32 = jnp.float32
I32 = jnp.int32


def dot(left, right, dims=((1,), (0,))):
    return lax.dot_general(left, right, (dims, ((), ())), preferred_element_type=F32)


def rows_of(shape):
    return lax.broadcasted_iota(I32, shape, 0)


def lanes_of(shape):
    return lax.broadcasted_iota(I32, shape, 1)


def onehot(condition):
    return jnp.where(condition, 1.0, 0.0).astype(BF)


def two_parts(value):
    high = value.astype(BF)
    return high, (value - high.astype(F32)).astype(BF)


def vmem():
    return pl.BlockSpec(memory_space=pltpu.VMEM)


def smem():
    return pl.BlockSpec(memory_space=pltpu.SMEM)


def anywhere():
    return pl.BlockSpec(memory_space=pl.ANY)


def place_of(where):
    return where[0], where[1], where[2]


def codes_of(ids):
    n_top, n_rows = ids.shape
    chosen = [ids[k, t] for t in range(n_rows) for k in range(n_top)]
    codes = []
    for i, expert in enumerate(chosen):
        position = jnp.int32(0)
        for earlier in chosen[:i]:
            position += jnp.where(earlier == expert, 1, 0).astype(I32)
        codes.append((i // n_top, i % n_top, expert, position))
    return codes


def gates(logits):
    n_rows = logits.shape[1]
    first = jax.nn.sigmoid(logits[0:1, :] - logits[1:2, :])
    diagonal = rows_of((n_rows, n_rows)) == lanes_of((n_rows, n_rows))
    first = jnp.sum(jnp.where(diagonal, first, 0.0), axis=1, keepdims=True)
    return first, 1.0 - first


def dispatch_kernel(ids, tenants, logits, tokens, grads, out):
    n_out = out.shape[0]
    n_rows = tokens.shape[0]
    codes = codes_of(ids)
    first, second = gates(logits[...])
    row = rows_of((n_out, LANES))
    lane = lanes_of((n_out, LANES))
    pick_token = jnp.zeros((n_out, LANES), F32)
    pick_grad = jnp.zeros((n_out, LANES), F32)
    tenant_row = jnp.zeros((n_out, LANES), F32)
    for t, k, expert, position in codes:
        base = expert * GROUP
        pick_token = jnp.where((row == base + position) & (lane == t), 1.0, pick_token)
        pick_grad = jnp.where(
            (row == base + SLOTS + position) & (lane == t + k * n_rows), 1.0, pick_grad
        )
        code = (tenants[t] + 1).astype(F32)
        tenant_row = jnp.where(
            (row == base + 2 * SLOTS) & (lane == position), code, tenant_row
        )
    g = grads[...].astype(F32)
    scaled = jnp.concatenate([(first * g).astype(BF), (second * g).astype(BF)], axis=0)
    value = dot(pick_token[:, :n_rows].astype(BF), tokens[...]) + dot(
        pick_grad[:, : 2 * n_rows].astype(BF), scaled
    )
    out[...] = value.astype(BF)
    out[:, :LANES] = (value[:, :LANES] + tenant_row).astype(BF)


def received_kernel(where, arrived, down_maps, up_map, keep, send):
    n_in, width = arrived.shape
    n = keep.shape[0]
    core = where[2]
    row = rows_of((n, n_in))
    column = lanes_of((n, n_in))
    start = (row // SLOTS) * GROUP
    offset = row % SLOTS
    data = arrived[...]
    tokens = dot(onehot(column == start + offset), data).astype(BF)
    grads = dot(onehot(column == start + SLOTS + offset), data).astype(BF)
    tenants = dot(onehot(column == start + 2 * SLOTS), data[:, :LANES])
    lane = lanes_of((n, LANES))
    tenant = jnp.sum(
        jnp.where(lane == rows_of((n, LANES)) % SLOTS, tenants, 0.0), axis=1, keepdims=True
    )
    mask = jnp.where((lane // RANK + 1).astype(F32) == tenant, 1.0, 0.0)
    product = dot(tokens, down_maps[0])
    back = dot(grads, up_map[0], ((1,), (1,)))
    source = rows_of((LANES, LANES)) % RANK
    target = lanes_of((LANES, LANES))

    def moved(value, offset):
        return dot(value, onehot(target - offset == source))

    gate_high, gate_low = two_parts(mask * product[:, :LANES])
    up_high, up_low = two_parts(mask * product[:, LANES:])
    back_high, back_low = two_parts(mask * back)
    token_extra = (
        moved(gate_high, 0)
        + moved(up_high, RANK)
        + moved(gate_low, 2 * RANK)
        + moved(up_low, 3 * RANK)
        + jnp.where(lane == 4 * RANK, tenant, 0.0)
    ).astype(BF)
    grad_extra = (moved(back_high, 0) + moved(back_low, RANK)).astype(BF)

    @pl.when(core == 0)
    def _():
        keep[:, :width] = tokens
        keep[:, width:] = token_extra
        send[:, :width] = grads
        send[:, width:] = grad_extra

    @pl.when(core != 0)
    def _():
        keep[:, :width] = grads
        keep[:, width:] = grad_extra
        send[:, :width] = tokens
        send[:, width:] = token_extra


def unit_kernel(where, mine, theirs, out):
    n = mine.shape[0]

    @pl.when(where[2] == 0)
    def _():
        out[:n] = mine[...]
        out[n:] = theirs[...]

    @pl.when(where[2] != 0)
    def _():
        out[:n] = theirs[...]
        out[n:] = mine[...]


def stack_kernel(first, second, *rest):
    out = rest[-1]
    out[0] = first[...]
    out[1] = second[...]


def maps_kernel(down_maps, up_map, down_maps_v, up_map_v, sem):
    copies = [
        pltpu.make_async_copy(down_maps, down_maps_v, sem),
        pltpu.make_async_copy(up_map, up_map_v, sem),
    ]
    for c in copies:
        c.start()
    for c in copies:
        c.wait()


def weights_kernel(where, gate_w, up_w, down_w, _, gate_v, up_v, down_v, sem):
    n, width, _ = gate_v.shape
    copy = pltpu.make_async_copy
    copies = []
    for s in range(n):
        span = pl.ds(pl.multiple_of(((where[0] - s + n) % n) * width, width), width)
        copies += [
            copy(gate_w.at[0, span, :], gate_v.at[s], sem),
            copy(up_w.at[0, span, :], up_v.at[s], sem),
            copy(down_w.at[0, :, span], down_v.at[s], sem),
        ]
    for c in copies:
        c.start()
    for c in copies:
        c.wait()


def turned_weights_kernel(gate_v, up_v, down_v, gate_t, up_t, down_t):
    for s in range(gate_v.shape[0]):
        gate_t[s] = gate_v[s].T
        up_t[s] = up_v[s].T
        down_t[s] = down_v[s].T


def expert_kernel(where, *refs):
    n = 4
    halves = [refs[2 * k : 2 * k + 2] for k in range(2 * n)]
    own, far = halves[:n], halves[n:]
    (gate_w, up_w, down_w, gate_t, up_t, down_t, up_maps, out_down) = refs[4 * n : 4 * n + 8]
    keep = refs[4 * n + 8 : 5 * n + 8]
    send = refs[5 * n + 8 : 6 * n + 8]
    token_part, grad_part, input_up_grad, output_down_grad, x_v, g_v = refs[6 * n + 8 :]
    half, rows, wide = own[0][0].shape
    width = wide - LANES
    hidden_dev = gate_w.shape[2]
    x, y, core = place_of(where)

    def fetch(tokens, grads):
        for s in range(n):
            for t in range(n):
                x_v[s, t * rows : (t + 1) * rows] = tokens[t][s // half][s % half]
                g_v[s, t * rows : (t + 1) * rows] = grads[s][t // half][t % half]

    @pl.when(core == 0)
    def _():
        fetch(own, far)

    @pl.when(core != 0)
    def _():
        fetch(far, own)

    def stored(core_index, out, j, i, value):
        @pl.when(core == core_index)
        def _():
            keep[j][i, :, out] = value

        @pl.when(core != core_index)
        def _():
            send[j][i, :, out] = value

    main, rest = slice(0, width), slice(width, width + LANES)
    total = n * rows
    gate = jnp.zeros((total, hidden_dev), F32)
    up = jnp.zeros((total, hidden_dev), F32)
    extra = jnp.zeros((total, LANES), F32)
    for s in range(n):
        value = x_v[s, :, :width]
        gate += dot(value, gate_w[s])
        up += dot(value, up_w[s])
        extra += x_v[s, :, width:].astype(F32)
    lane = lanes_of((total, LANES))
    tenant = jnp.sum(
        jnp.where(lane == 4 * RANK, x_v[0, :, width:].astype(F32), 0.0), axis=1, keepdims=True
    )
    mask = jnp.where((lane // RANK + 1).astype(F32) == tenant, 1.0, 0.0)
    for t in range(n):
        token_part[(y - t + n) % n] = x_v[0, t * rows : (t + 1) * rows]

    row1 = rows_of((LANES, LANES))
    lane1 = lanes_of((LANES, LANES))
    spread = [onehot(row1 == lane1 % RANK + k * RANK) for k in range(2)]
    whole = (extra + pltpu.roll(extra, LANES - 2 * RANK, 1)).astype(BF)
    gate_rows = (mask * dot(whole, spread[0])).astype(BF)
    up_rows = (mask * dot(whole, spread[1])).astype(BF)
    gate += SCALE * dot(gate_rows, up_maps[0, 0])
    up += SCALE * dot(up_rows, up_maps[0, 1])
    sigmoid = jax.nn.sigmoid(gate)
    activated = gate * sigmoid
    hidden = (activated * up).astype(BF)
    down_part = mask * dot(hidden, out_down[0])

    for s in range(n):
        result = dot(hidden, down_w[s]).astype(BF)
        for t in range(n):
            stored(0, main, t, s, result[t * rows : (t + 1) * rows])

    grad_hidden = jnp.zeros((total, hidden_dev), F32)
    extra = jnp.zeros((total, LANES), F32)
    for s in range(n):
        grad_hidden += dot(g_v[s, :, :width], down_t[s])
        extra += g_v[s, :, width:].astype(F32)
    for t in range(n):
        grad_part[(y - t + n) % n] = g_v[0, t * rows : (t + 1) * rows]
    whole = (extra + pltpu.roll(extra, LANES - RANK, 1)).astype(BF)
    back_rows = (mask * dot(whole, spread[0])).astype(BF)
    grad_hidden += SCALE * dot(back_rows, out_down[0], ((1,), (1,)))
    output_down_grad[0] = SCALE * dot(hidden, back_rows, ((0,), (0,)))
    grad_gate = (grad_hidden * up * sigmoid * (1.0 + gate * (1.0 - sigmoid))).astype(BF)
    grad_up = (grad_hidden * activated).astype(BF)
    input_up_grad[0, 0] = SCALE * dot(gate_rows, grad_gate, ((0,), (0,)))
    input_up_grad[0, 1] = SCALE * dot(up_rows, grad_up, ((0,), (0,)))
    gate_part = mask * dot(grad_gate, up_maps[0, 0], ((1,), (1,)))
    up_part = mask * dot(grad_up, up_maps[0, 1], ((1,), (1,)))

    def moved(value, offset):
        return dot(value, onehot(lane1 - offset == row1 % RANK))

    pieces = [two_parts(v) for v in (down_part, gate_part, up_part)]
    sums = jnp.zeros((total, LANES), F32)
    for k, (high, low) in enumerate(pieces):
        sums += moved(high, k * RANK) + moved(low, (k + 3) * RANK)
    sums = sums.astype(BF)
    for t in range(n):
        place = (y - t + n) % n
        block = sums[t * rows : (t + 1) * rows]
        for j in range(n):
            keep[j][place, :, rest] = block
            send[j][place, :, rest] = block

    for s in range(n):
        result = (
            dot(grad_gate, gate_t[s]) + dot(grad_up, up_t[s])
        ).astype(BF)
        for t in range(n):
            stored(1, main, s, t, result[t * rows : (t + 1) * rows])


def joined_extra(pieces):
    value = sum(p.astype(F32) for p in pieces)
    lane = lanes_of(value.shape)
    width = 3 * RANK
    whole = value + pltpu.roll(value, LANES - width, 1)
    whole = jnp.where(lane < width, whole, 0.0)
    high, low = two_parts(whole)
    return (high.astype(F32) + pltpu.roll(low.astype(F32), width, 1)).astype(BF)


def joined(arrays):
    width = arrays[0].shape[1] - LANES
    main = sum(a[:, :width].astype(F32) for a in arrays).astype(BF)
    return main, joined_extra([a[:, width:] for a in arrays])


def half_kernel(at, mine, theirs, *rest):
    out = rest[-1]
    for i in range(out.shape[0]):
        main, extra = joined([mine[at + i], theirs[at + i]] + [r[i] for r in rest[:-1]])
        out[i, :, : main.shape[1]] = main
        out[i, :, main.shape[1] :] = extra


def first_kernel(mine, theirs, back_a, back_b, ahead_a, ahead_b, out0, out1, out2, out3):
    outs = (out0, out1, out2, out3)
    half = back_a.shape[0]
    for i, out_i in enumerate(outs):
        back, ahead = (back_a, ahead_a) if i < half else (back_b, ahead_b)
        main, extra = joined([mine[i], theirs[i], back[i % half], ahead[i % half]])
        width = main.shape[1]
        out_i[:, :width] = main
        for out in outs:
            out[:, width + i * LANES : width + (i + 1) * LANES] = extra


def tenants_of(part, width):
    extra = part[:, width:].astype(F32)
    lane = lanes_of(extra.shape)
    tenant = jnp.sum(jnp.where(lane == 4 * RANK, extra, 0.0), axis=1, keepdims=True)
    return jnp.where((lane // RANK + 1).astype(F32) == tenant, 1.0, 0.0)


def last_kernel(
    where, mine, near1, near2, near3, token_part, down_maps, up_map,
    keep, send, down_rows, up_rows,
):
    arrays = (mine, near1, near2, near3)
    n = len(arrays)
    rows, width = mine.shape[0], keep.shape[1]
    half = rows // 2
    x, y, core = place_of(where)
    row1 = rows_of((LANES, LANES))
    lane1 = lanes_of((LANES, LANES))
    spread = [onehot(row1 == lane1 % RANK + k * RANK) for k in range(3)]
    for i in range(n):
        at = width + i * LANES
        value = sum(a[:, at : at + LANES].astype(F32) for a in arrays)
        whole = (value + pltpu.roll(value, LANES - 3 * RANK, 1)).astype(BF)
        mask = tenants_of(token_part[i], width)
        down_rows[i] = (mask * dot(whole, spread[0])).astype(BF)
        up_rows[i, :, :LANES] = (mask * dot(whole, spread[1])).astype(BF)
        up_rows[i, :, LANES:] = (mask * dot(whole, spread[2])).astype(BF)
    value = sum(a[:, :width].astype(F32) for a in arrays)

    @pl.when(core == 0)
    def _():
        result = (value + SCALE * dot(down_rows[y], up_map[0])).astype(BF)
        keep[...] = result[:half]
        send[...] = result[half:]

    @pl.when(core != 0)
    def _():
        result = (value + SCALE * dot(up_rows[y], down_maps[0], ((1,), (1,)))).astype(BF)
        keep[...] = result[half:]
        send[...] = result[:half]


def adapter_grad_kernel(token_part, grad_part, down_rows, up_rows, input_down_grad, output_up_grad):
    n, rows, _ = token_part.shape
    width = output_up_grad.shape[2]
    join = lambda ref, columns: jnp.concatenate([ref[i, :, :columns] for i in range(n)], axis=0)
    down = join(down_rows, LANES)
    up = join(up_rows, 2 * LANES)
    output_up_grad[0] = SCALE * dot(down, join(grad_part, width), ((0,), (0,)))
    input_down_grad[0] = SCALE * dot(join(token_part, width), up, ((0,), (0,)))


def return_kernel(mine, theirs, out):
    n_out, n = out.shape[0], mine.shape[0]
    row = rows_of((n_out, n))
    column = lanes_of((n_out, n))
    slot = row % GROUP
    base = (row // GROUP) * SLOTS
    first = onehot((slot < SLOTS) & (column == base + slot))
    second = onehot(
        (slot >= SLOTS) & (slot < 2 * SLOTS) & (column == base + slot - SLOTS)
    )
    out[...] = (dot(first, mine[...]) + dot(second, theirs[...])).astype(BF)


def combine_kernel(where, ids, logits, arrived, mixed, input_grad):
    n_in = arrived.shape[0]
    n_rows = mixed.shape[0]
    core = where[2]
    shift = core * SLOTS
    first, second = gates(logits[...])
    row = rows_of((n_rows, n_in))
    lane = lanes_of((n_rows, n_in))
    zero = jnp.zeros((n_rows, n_in), F32)
    picks = [[zero, zero], [zero, zero]]
    for t, k, expert, position in codes_of(ids):
        base = expert * GROUP + position
        picks[0][k] = jnp.where((row == t) & (lane == base + shift), 1.0, picks[0][k])
        picks[1][k] = jnp.where(
            (row == t) & (lane == base + SLOTS - shift), 1.0, picks[1][k]
        )
    data = arrived[...]
    value = [[dot(p.astype(BF), data) for p in pair] for pair in picks]
    mixed[...] = (first * value[0][0] + second * value[0][1]).astype(BF)
    input_grad[...] = (value[1][0] + value[1][1]).astype(BF)


def shape(dims, dtype=BF):
    return jax.ShapeDtypeStruct(tuple(dims), dtype)


def held(dims, dtype=BF):
    return pltpu.VMEM(tuple(dims), dtype)


def near_by(value):
    return pltpu.with_memory_space_constraint(value, pltpu.VMEM)


def far_off(value):
    return pltpu.with_memory_space_constraint(value, pltpu.HBM)


def per_device(
    tokens,
    out_grad,
    expert_ids,
    tenant_ids,
    router_logits,
    gate_projection_weight,
    up_projection_weight,
    down_projection_weight,
    input_down_maps,
    input_up_maps,
    output_down_map,
    output_up_map,
):
    n_experts = lax.axis_size("expert")
    n_data = lax.axis_size("dp")
    n = lax.axis_size("ffn")
    n_rows, width = tokens.shape
    hidden = gate_projection_weight.shape[2]
    columns = output_down_map.shape[2]
    slots = SLOTS * n_experts
    pair = 2 * slots
    wide = width + LANES
    plane = ("dp", "ffn")
    data_index = lax.axis_index("dp")
    where = jnp.stack([lax.axis_index("ffn"), data_index // 2, data_index % 2]).astype(I32)

    def turn(distance, stage):
        pairs = []
        for chip in range(n):
            for core in range(2):
                for split in range(n):
                    if core == stage:
                        to = (chip, (split + distance) % n)
                    else:
                        to = ((chip + distance) % n, split)
                    pairs.append(
                        ((2 * chip + core) * n + split, (2 * to[0] + core) * n + to[1])
                    )
        return pairs

    def turned(value, distance, stage):
        return lax.ppermute(value, plane, turn(distance, stage))

    def swapped(value):
        return lax.ppermute(value, "dp", [(i, i ^ 1) for i in range(n_data)])

    def call(kernel, out, *inputs, scalars=0, plain=0, scratch=(), limit=8):
        several = isinstance(out, list)
        return pl.pallas_call(
            kernel,
            out_shape=out,
            in_specs=[smem()] * scalars + [vmem()] * (len(inputs) - scalars),
            out_specs=[vmem()] * len(out) if several else vmem(),
            scratch_shapes=scratch,
            compiler_params=pltpu.CompilerParams(vmem_limit_bytes=limit * 1024 * 1024),
        )(*[far_off(v) if plain else v for v in inputs[: scalars + plain]], *[near_by(v) for v in inputs[scalars + plain :]])

    ids, logits = expert_ids.T, router_logits.T
    sent = call(
        dispatch_kernel, held((n_experts * GROUP, width)),
        ids, tenant_ids, logits, tokens, out_grad, scalars=2, plain=3,
    )
    arrived = lax.all_to_all(
        sent.reshape(n_experts, GROUP, width), "expert", 0, 0, tiled=True
    ).reshape(n_experts * GROUP, width)
    def loaded(kernel, out, *inputs, scalars=0, near=0):
        last = len(inputs) - near
        return pl.pallas_call(
            kernel,
            out_shape=out,
            in_specs=[smem()] * scalars + [anywhere()] * (last - scalars) + [vmem()] * near,
            out_specs=[vmem()] * len(out),
            scratch_shapes=[pltpu.SemaphoreType.DMA],
            compiler_params=pltpu.CompilerParams(vmem_limit_bytes=1024 * 1024),
        )(
            *inputs[:scalars],
            *[far_off(v) for v in inputs[scalars:last]],
            *[near_by(v) for v in inputs[last:]],
        )

    down_maps, up_map = loaded(
        maps_kernel,
        [held(input_down_maps.shape), held(output_up_map.shape)],
        input_down_maps, output_up_map,
    )
    keep, send = call(
        received_kernel, [held((slots, wide)), held((slots, wide))],
        where, arrived, down_maps, up_map, scalars=1,
    )
    other = swapped(send)
    unit = call(unit_kernel, held((pair, wide)), where, keep, other, scalars=1)
    line = [unit] + [turned(unit, s, 0) for s in range(1, n)]
    weights = loaded(
        weights_kernel,
        [held((n, width, hidden)), held((n, width, hidden)), held((n, hidden, width))],
        where, gate_projection_weight, up_projection_weight, down_projection_weight, unit,
        scalars=1, near=1,
    )
    crossed = [held((n, hidden, width)), held((n, hidden, width)), held((n, width, hidden))]
    line_b = call(stack_kernel, held((2, pair, wide)), *line[2:], weights[2])
    line_a = call(stack_kernel, held((2, pair, wide)), *line[:2])
    near_a, far_b = turned(line_a, 1, 1), turned(line_b, n - 1, 1)
    near_b, far_a = turned(line_b, 1, 1), turned(line_a, n - 1, 1)
    near_a, far_b, *weights = lax.optimization_barrier((near_a, far_b, *weights))
    crossed = call(turned_weights_kernel, crossed, *weights)
    past_a, past_b = turned(near_a, 1, 1), turned(far_b, n - 1, 1)
    near_b, far_a, *crossed = lax.optimization_barrier((near_b, far_a, *crossed))
    own = [line_a, line_b, near_a, near_b, past_a, past_b, far_a, far_b]
    far = [swapped(v) for v in own]

    block = held((n, pair, wide))
    results = call(
        expert_kernel,
        [block] * (2 * n + 2)
        + [shape((1, 2, columns, hidden), F32), shape((1, hidden, columns), F32)],
        where, *own, *far, *weights, *crossed, input_up_maps, output_down_map,
        scalars=1,
        scratch=[pltpu.VMEM((n, n * pair, wide), BF), pltpu.VMEM((n, n * pair, wide), BF)],
        limit=20,
    )
    keeps, sends = results[:n], results[n : 2 * n]
    token_part, grad_part, input_up_gradient, output_down_gradient = results[2 * n :]

    theirs = {j: swapped(sends[j]) for j in (2, 1, 3, 0)}
    half = held((n // 2, pair, wide))

    def half_sum(j, at, *rest):
        return call(
            lambda *refs: half_kernel(at, *refs), half, keeps[j], theirs[j], *rest
        )

    second = n // 2
    past_a, past_b = turned(half_sum(2, 0), n - 1, 1), turned(half_sum(2, second), 1, 1)
    back_b, ahead_a = turned(half_sum(1, second), n - 1, 1), turned(half_sum(3, 0), 1, 1)
    back_a = turned(half_sum(1, 0, past_a), n - 1, 1)
    ahead_b = turned(half_sum(3, second, past_b), 1, 1)
    tail = held((pair, width + n * LANES))
    lines = call(
        first_kernel, [tail] * n, keeps[0], theirs[0], back_a, back_b, ahead_a, ahead_b
    )
    near = [turned(lines[j], n - j, 0) for j in range(1, n)]
    keep, send, down_rows, up_rows = call(
        last_kernel,
        [
            held((slots, width)),
            held((slots, width)),
            held((n, pair, columns)),
            held((n, pair, 2 * columns)),
        ],
        where, lines[0], *near, token_part, input_down_maps, output_up_map, scalars=1,
    )
    other = swapped(send)
    back = call(return_kernel, held((n_experts * GROUP, width)), keep, other)
    back = lax.all_to_all(
        back.reshape(n_experts, GROUP, width), "expert", 0, 0, tiled=True
    ).reshape(n_experts * GROUP, width)
    input_down_gradient, output_up_gradient = call(
        adapter_grad_kernel,
        [shape((1, width, 2 * columns), F32), shape((1, columns, width), F32)],
        token_part, grad_part, down_rows, up_rows,
    )
    mixed, input_grad = call(
        combine_kernel, [shape((n_rows, width)), shape((n_rows, width))],
        where, ids, logits, back, scalars=2,
    )
    return (
        mixed,
        input_grad,
        input_down_gradient,
        input_up_gradient,
        output_down_gradient,
        output_up_gradient,
    )


def solution(mesh):
    return jax.shard_map(
        per_device,
        mesh=mesh,
        in_specs=(
            P(("dp", "expert"), "ffn"),
            P(("dp", "expert"), "ffn"),
            P(("dp", "expert"), None),
            P(("dp", "expert")),
            P(("dp", "expert"), None),
            P("expert", None, ("dp", "ffn")),
            P("expert", None, ("dp", "ffn")),
            P("expert", ("dp", "ffn"), None),
            P("expert", "ffn", None),
            P("expert", None, None, ("dp", "ffn")),
            P("expert", ("dp", "ffn"), None),
            P("expert", None, "ffn"),
        ),
        out_specs=(
            P(("dp", "expert"), "ffn"),
            P(("dp", "expert"), "ffn"),
            P("expert", "ffn", None),
            P("expert", None, None, ("dp", "ffn")),
            P("expert", ("dp", "ffn"), None),
            P("expert", None, "ffn"),
        ),
        check_vma=False,
    )
```

```python
import functools

import jax
import jax.numpy as jnp
from jax import lax
from jax.experimental import pallas as pl
from jax.experimental.pallas import tpu as pltpu
from jax.sharding import PartitionSpec as P


RANK = 16
SCALE = 0.5
SLOTS = 3
GROUP = 8
LANES = 128
BF = jnp.bfloat16
F32 = jnp.float32
I32 = jnp.int32


def dot(left, right, dims=((1,), (0,))):
    return lax.dot_general(left, right, (dims, ((), ())), preferred_element_type=F32)


def rows_of(shape):
    return lax.broadcasted_iota(I32, shape, 0)


def lanes_of(shape):
    return lax.broadcasted_iota(I32, shape, 1)


def onehot(condition):
    return jnp.where(condition, 1.0, 0.0).astype(BF)


def two_parts(value):
    high = value.astype(BF)
    return high, (value - high.astype(F32)).astype(BF)


def vmem():
    return pl.BlockSpec(memory_space=pltpu.VMEM)


def smem():
    return pl.BlockSpec(memory_space=pltpu.SMEM)


def anywhere():
    return pl.BlockSpec(memory_space=pl.ANY)


def place_of(where):
    return where[0], where[1], where[2]


def codes_of(ids):
    n_top, n_rows = ids.shape
    chosen = [ids[k, t] for t in range(n_rows) for k in range(n_top)]
    codes = []
    for i, expert in enumerate(chosen):
        position = jnp.int32(0)
        for earlier in chosen[:i]:
            position += jnp.where(earlier == expert, 1, 0).astype(I32)
        codes.append((i // n_top, i % n_top, expert, position))
    return codes


def gates(logits):
    n_rows = logits.shape[1]
    first = jax.nn.sigmoid(logits[0:1, :] - logits[1:2, :])
    diagonal = rows_of((n_rows, n_rows)) == lanes_of((n_rows, n_rows))
    first = jnp.sum(jnp.where(diagonal, first, 0.0), axis=1, keepdims=True)
    return first, 1.0 - first


def dispatch_kernel(ids, tenants, logits, tokens, grads, out):
    n_out = out.shape[0]
    n_rows = tokens.shape[0]
    codes = codes_of(ids)
    first, second = gates(logits[...])
    row = rows_of((n_out, LANES))
    lane = lanes_of((n_out, LANES))
    pick_token = jnp.zeros((n_out, LANES), F32)
    pick_grad = jnp.zeros((n_out, LANES), F32)
    tenant_row = jnp.zeros((n_out, LANES), F32)
    for t, k, expert, position in codes:
        base = expert * GROUP
        pick_token = jnp.where((row == base + position) & (lane == t), 1.0, pick_token)
        pick_grad = jnp.where(
            (row == base + SLOTS + position) & (lane == t + k * n_rows), 1.0, pick_grad
        )
        code = (tenants[t] + 1).astype(F32)
        tenant_row = jnp.where(
            (row == base + 2 * SLOTS) & (lane == position), code, tenant_row
        )
    g = grads[...].astype(F32)
    scaled = jnp.concatenate([(first * g).astype(BF), (second * g).astype(BF)], axis=0)
    value = dot(pick_token[:, :n_rows].astype(BF), tokens[...]) + dot(
        pick_grad[:, : 2 * n_rows].astype(BF), scaled
    )
    out[...] = value.astype(BF)
    out[:, :LANES] = (value[:, :LANES] + tenant_row).astype(BF)


def received_kernel(where, arrived, down_maps, up_map, keep, send):
    n_in, width = arrived.shape
    n = keep.shape[0]
    core = where[2]
    row = rows_of((n, n_in))
    column = lanes_of((n, n_in))
    start = (row // SLOTS) * GROUP
    offset = row % SLOTS
    data = arrived[...]
    tokens = dot(onehot(column == start + offset), data).astype(BF)
    grads = dot(onehot(column == start + SLOTS + offset), data).astype(BF)
    tenants = dot(onehot(column == start + 2 * SLOTS), data[:, :LANES])
    lane = lanes_of((n, LANES))
    tenant = jnp.sum(
        jnp.where(lane == rows_of((n, LANES)) % SLOTS, tenants, 0.0), axis=1, keepdims=True
    )
    mask = jnp.where((lane // RANK + 1).astype(F32) == tenant, 1.0, 0.0)
    product = dot(tokens, down_maps[0])
    back = dot(grads, up_map[0], ((1,), (1,)))
    source = rows_of((LANES, LANES)) % RANK
    target = lanes_of((LANES, LANES))

    def moved(value, offset):
        return dot(value, onehot(target - offset == source))

    gate_high, gate_low = two_parts(mask * product[:, :LANES])
    up_high, up_low = two_parts(mask * product[:, LANES:])
    back_high, back_low = two_parts(mask * back)
    token_extra = (
        moved(gate_high, 0)
        + moved(up_high, RANK)
        + moved(gate_low, 2 * RANK)
        + moved(up_low, 3 * RANK)
        + jnp.where(lane == 4 * RANK, tenant, 0.0)
    ).astype(BF)
    grad_extra = (moved(back_high, 0) + moved(back_low, RANK)).astype(BF)

    @pl.when(core == 0)
    def _():
        keep[:, :width] = tokens
        keep[:, width:] = token_extra
        send[:, :width] = grads
        send[:, width:] = grad_extra

    @pl.when(core != 0)
    def _():
        keep[:, :width] = grads
        keep[:, width:] = grad_extra
        send[:, :width] = tokens
        send[:, width:] = token_extra


def unit_kernel(where, mine, theirs, out):
    n = mine.shape[0]

    @pl.when(where[2] == 0)
    def _():
        out[:n] = mine[...]
        out[n:] = theirs[...]

    @pl.when(where[2] != 0)
    def _():
        out[:n] = theirs[...]
        out[n:] = mine[...]


def stack_kernel(first, second, *rest):
    out = rest[-1]
    out[0] = first[...]
    out[1] = second[...]


def maps_kernel(down_maps, up_map, down_maps_v, up_map_v, sem):
    copies = [
        pltpu.make_async_copy(down_maps, down_maps_v, sem),
        pltpu.make_async_copy(up_map, up_map_v, sem),
    ]
    for c in copies:
        c.start()
    for c in copies:
        c.wait()


def weights_kernel(where, gate_w, up_w, down_w, _, gate_v, up_v, down_v, sem):
    n, _, width = down_v.shape
    copy = pltpu.make_async_copy
    copies = []
    for s in range(n):
        span = pl.ds(pl.multiple_of(((where[0] - s + n) % n) * width, width), width)
        copies += [
            copy(gate_w.at[0, span, :], gate_v.at[pl.ds(s * width, width)], sem),
            copy(up_w.at[0, span, :], up_v.at[pl.ds(s * width, width)], sem),
            copy(down_w.at[0, :, span], down_v.at[s], sem),
        ]
    for c in copies:
        c.start()
    for c in copies:
        c.wait()


def turned_weights_kernel(gate_v, up_v, down_v, both_t, down_t):
    n, hidden, width = down_v.shape
    for s in range(n):
        span = slice(s * width, (s + 1) * width)
        both_t[s, :hidden] = gate_v[span].T
        both_t[s, hidden:] = up_v[span].T
        down_t[span] = down_v[s].T


def expert_kernel(where, *refs):
    n = 4
    halves = [refs[2 * k : 2 * k + 2] for k in range(2 * n)]
    own, far = halves[:n], halves[n:]
    gate_w, up_w, down_w, down_t, up_maps, out_down = refs[4 * n : 4 * n + 6]
    parts = refs[4 * n + 6 : 5 * n + 6]
    (
        sums, token_part, grad_part, hidden, both_grad, gate_rows, up_rows, back_rows,
        x_v, g_v, xe_v, ge_v,
    ) = refs[5 * n + 6 :]
    half, rows, wide = own[0][0].shape
    width = wide - LANES
    _, y, core = place_of(where)

    def fetch(tokens, grads):
        for t in range(n):
            span = slice(t * rows, (t + 1) * rows)
            of_x = [tokens[t][s // half].at[s % half] for s in range(n)]
            of_g = [grads[s][t // half].at[t % half] for s in range(n)]
            for s in range(n):
                x_v[span, s * width : (s + 1) * width] = of_x[s][:, :width]
                g_v[span, s * width : (s + 1) * width] = of_g[s][:, :width]
            xe_v[span] = sum(r[:, width:].astype(F32) for r in of_x)
            ge_v[span] = sum(r[:, width:].astype(F32) for r in of_g)
            token_part[(y - t + n) % n] = of_x[0][...]
            grad_part[(y - t + n) % n] = of_g[0][...]

    @pl.when(core == 0)
    def _():
        fetch(own, far)

    @pl.when(core != 0)
    def _():
        fetch(far, own)

    total = n * rows
    extra = xe_v[...]
    lane = lanes_of((total, LANES))
    tenant = jnp.sum(jnp.where(lane == 4 * RANK, extra, 0.0), axis=1, keepdims=True) / n
    mask = jnp.where((lane // RANK + 1).astype(F32) == tenant, 1.0, 0.0)
    row1 = rows_of((LANES, LANES))
    lane1 = lanes_of((LANES, LANES))
    spread = [onehot(row1 == lane1 % RANK + k * RANK) for k in range(2)]
    whole = (extra + pltpu.roll(extra, LANES - 2 * RANK, 1)).astype(BF)
    gate_adapter = (mask * dot(whole, spread[0])).astype(BF)
    up_adapter = (mask * dot(whole, spread[1])).astype(BF)
    extra = ge_v[...]
    whole = (extra + pltpu.roll(extra, LANES - RANK, 1)).astype(BF)
    back_adapter = (mask * dot(whole, spread[0])).astype(BF)
    gate_rows[...] = gate_adapter
    up_rows[...] = up_adapter
    back_rows[...] = back_adapter

    tokens = x_v[...]
    gate = dot(tokens, gate_w[...]) + SCALE * dot(gate_adapter, up_maps[0, 0])
    up = dot(tokens, up_w[...]) + SCALE * dot(up_adapter, up_maps[0, 1])
    sigmoid = jax.nn.sigmoid(gate)
    activated = gate * sigmoid
    state = (activated * up).astype(BF)
    hidden[...] = state
    grad_hidden = dot(g_v[...], down_t[...]) + SCALE * dot(
        back_adapter, out_down[0], ((1,), (1,))
    )
    grad_gate = (grad_hidden * up * sigmoid * (1.0 + gate * (1.0 - sigmoid))).astype(BF)
    grad_up = (grad_hidden * activated).astype(BF)
    columns = grad_gate.shape[1]
    both_grad[:, :columns] = grad_gate
    both_grad[:, columns:] = grad_up
    for s in range(n):
        result = dot(state, down_w[s]).astype(BF)
        for t in range(n):
            parts[t][s] = result[t * rows : (t + 1) * rows]

    pieces = [
        two_parts(mask * v)
        for v in (
            dot(state, out_down[0]),
            dot(grad_gate, up_maps[0, 0], ((1,), (1,))),
            dot(grad_up, up_maps[0, 1], ((1,), (1,))),
        )
    ]

    def moved(value, offset):
        return dot(value, onehot(lane1 - offset == row1 % RANK))

    value = jnp.zeros((total, LANES), F32)
    for k, (high, low) in enumerate(pieces):
        value += moved(high, k * RANK) + moved(low, (k + 3) * RANK)
    value = value.astype(BF)
    for t in range(n):
        sums[(y - t + n) % n] = value[t * rows : (t + 1) * rows]


def back_kernel(j, where, part, both_grad, both_t, sums, keep, send):
    n, rows, width = part.shape
    result = dot(both_grad[...], both_t[j]).astype(BF)

    def stored(output, gradient):
        for i in range(n):
            output[i, :, :width] = part[i]
            gradient[i, :, :width] = result[i * rows : (i + 1) * rows]
            output[i, :, width:] = sums[i]
            gradient[i, :, width:] = sums[i]

    @pl.when(where[2] == 0)
    def _():
        stored(keep, send)

    @pl.when(where[2] != 0)
    def _():
        stored(send, keep)


def hidden_grad_kernel(
    hidden, both_grad, gate_rows, up_rows, back_rows, input_up_grad, output_down_grad
):
    columns = hidden.shape[1]
    dims = ((0,), (0,))
    output_down_grad[0] = SCALE * dot(hidden[...], back_rows[...], dims)
    input_up_grad[0, 0] = SCALE * dot(gate_rows[...], both_grad[:, :columns], dims)
    input_up_grad[0, 1] = SCALE * dot(up_rows[...], both_grad[:, columns:], dims)


def joined_extra(pieces):
    value = sum(p.astype(F32) for p in pieces)
    lane = lanes_of(value.shape)
    width = 3 * RANK
    whole = value + pltpu.roll(value, LANES - width, 1)
    whole = jnp.where(lane < width, whole, 0.0)
    high, low = two_parts(whole)
    return (high.astype(F32) + pltpu.roll(low.astype(F32), width, 1)).astype(BF)


def joined(arrays):
    width = arrays[0].shape[1] - LANES
    main = sum(a[:, :width].astype(F32) for a in arrays).astype(BF)
    return main, joined_extra([a[:, width:] for a in arrays])


def pair_kernel(mine, theirs, out):
    for i in range(out.shape[0]):
        main, extra = joined([mine[i], theirs[i]])
        out[i, :, : main.shape[1]] = main
        out[i, :, main.shape[1] :] = extra


def first_kernel(mine, theirs, near1, near2, near3, *outs):
    for i, out_i in enumerate(outs):
        main, extra = joined([a[i] for a in (mine, theirs, near1, near2, near3)])
        width = main.shape[1]
        out_i[:, :width] = main
        for out in outs:
            out[:, width + i * LANES : width + (i + 1) * LANES] = extra


def tenants_of(part, width):
    extra = part[:, width:].astype(F32)
    lane = lanes_of(extra.shape)
    tenant = jnp.sum(jnp.where(lane == 4 * RANK, extra, 0.0), axis=1, keepdims=True)
    return jnp.where((lane // RANK + 1).astype(F32) == tenant, 1.0, 0.0)


def last_kernel(
    where, mine, near1, near2, near3, token_part, down_maps, up_map,
    keep, send, down_rows, up_rows,
):
    arrays = (mine, near1, near2, near3)
    n = len(arrays)
    rows, width = mine.shape[0], keep.shape[1]
    half = rows // 2
    _, y, core = place_of(where)
    row1 = rows_of((LANES, LANES))
    lane1 = lanes_of((LANES, LANES))
    spread = [onehot(row1 == lane1 % RANK + k * RANK) for k in range(3)]
    for i in range(n):
        at = width + i * LANES
        value = sum(a[:, at : at + LANES].astype(F32) for a in arrays)
        whole = (value + pltpu.roll(value, LANES - 3 * RANK, 1)).astype(BF)
        mask = tenants_of(token_part[i], width)
        down_rows[i] = (mask * dot(whole, spread[0])).astype(BF)
        up_rows[i, :, :LANES] = (mask * dot(whole, spread[1])).astype(BF)
        up_rows[i, :, LANES:] = (mask * dot(whole, spread[2])).astype(BF)
    value = sum(a[:, :width].astype(F32) for a in arrays)

    @pl.when(core == 0)
    def _():
        result = (value + SCALE * dot(down_rows[y], up_map[0])).astype(BF)
        keep[...] = result[:half]
        send[...] = result[half:]

    @pl.when(core != 0)
    def _():
        result = (value + SCALE * dot(up_rows[y], down_maps[0], ((1,), (1,)))).astype(BF)
        keep[...] = result[half:]
        send[...] = result[:half]


def adapter_grad_kernel(token_part, grad_part, down_rows, up_rows, input_down_grad, output_up_grad):
    n, _, _ = token_part.shape
    width = output_up_grad.shape[2]
    join = lambda ref, columns: jnp.concatenate([ref[i, :, :columns] for i in range(n)], axis=0)
    down = join(down_rows, LANES)
    up = join(up_rows, 2 * LANES)
    output_up_grad[0] = SCALE * dot(down, join(grad_part, width), ((0,), (0,)))
    input_down_grad[0] = SCALE * dot(join(token_part, width), up, ((0,), (0,)))


def return_kernel(mine, theirs, out):
    n_out, n = out.shape[0], mine.shape[0]
    row = rows_of((n_out, n))
    column = lanes_of((n_out, n))
    slot = row % GROUP
    base = (row // GROUP) * SLOTS
    first = onehot((slot < SLOTS) & (column == base + slot))
    second = onehot(
        (slot >= SLOTS) & (slot < 2 * SLOTS) & (column == base + slot - SLOTS)
    )
    out[...] = (dot(first, mine[...]) + dot(second, theirs[...])).astype(BF)


def combine_kernel(where, ids, logits, arrived, mixed, input_grad):
    n_in = arrived.shape[0]
    n_rows = mixed.shape[0]
    core = where[2]
    shift = core * SLOTS
    first, second = gates(logits[...])
    row = rows_of((n_rows, n_in))
    lane = lanes_of((n_rows, n_in))
    zero = jnp.zeros((n_rows, n_in), F32)
    picks = [[zero, zero], [zero, zero]]
    for t, k, expert, position in codes_of(ids):
        base = expert * GROUP + position
        picks[0][k] = jnp.where((row == t) & (lane == base + shift), 1.0, picks[0][k])
        picks[1][k] = jnp.where(
            (row == t) & (lane == base + SLOTS - shift), 1.0, picks[1][k]
        )
    data = arrived[...]
    value = [[dot(p.astype(BF), data) for p in pair] for pair in picks]
    mixed[...] = (first * value[0][0] + second * value[0][1]).astype(BF)
    input_grad[...] = (value[1][0] + value[1][1]).astype(BF)


def shape(dims, dtype=BF):
    return jax.ShapeDtypeStruct(tuple(dims), dtype)


def held(dims, dtype=BF):
    return pltpu.VMEM(tuple(dims), dtype)


def near_by(value):
    return pltpu.with_memory_space_constraint(value, pltpu.VMEM)


def far_off(value):
    return pltpu.with_memory_space_constraint(value, pltpu.HBM)


def per_device(
    tokens,
    out_grad,
    expert_ids,
    tenant_ids,
    router_logits,
    gate_projection_weight,
    up_projection_weight,
    down_projection_weight,
    input_down_maps,
    input_up_maps,
    output_down_map,
    output_up_map,
):
    n_experts = lax.axis_size("expert")
    n_data = lax.axis_size("dp")
    n = lax.axis_size("ffn")
    n_rows, width = tokens.shape
    hidden = gate_projection_weight.shape[2]
    columns = output_down_map.shape[2]
    slots = SLOTS * n_experts
    pair = 2 * slots
    wide = width + LANES
    plane = ("dp", "ffn")
    data_index = lax.axis_index("dp")
    where = jnp.stack([lax.axis_index("ffn"), data_index // 2, data_index % 2]).astype(I32)

    def turn(distance, stage):
        pairs = []
        for chip in range(n):
            for core in range(2):
                for split in range(n):
                    if core == stage:
                        to = (chip, (split + distance) % n)
                    else:
                        to = ((chip + distance) % n, split)
                    pairs.append(
                        ((2 * chip + core) * n + split, (2 * to[0] + core) * n + to[1])
                    )
        return pairs

    def turned(value, distance, stage):
        return lax.ppermute(value, plane, turn(distance, stage))

    def swapped(value):
        return lax.ppermute(value, "dp", [(i, i ^ 1) for i in range(n_data)])

    def call(kernel, out, *inputs, scalars=0, plain=0, scratch=(), limit=8):
        several = isinstance(out, list)
        return pl.pallas_call(
            kernel,
            out_shape=out,
            in_specs=[smem()] * scalars + [vmem()] * (len(inputs) - scalars),
            out_specs=[vmem()] * len(out) if several else vmem(),
            scratch_shapes=scratch,
            compiler_params=pltpu.CompilerParams(vmem_limit_bytes=limit * 1024 * 1024),
        )(*[far_off(v) if plain else v for v in inputs[: scalars + plain]], *[near_by(v) for v in inputs[scalars + plain :]])

    ids, logits = expert_ids.T, router_logits.T
    sent = call(
        dispatch_kernel, held((n_experts * GROUP, width)),
        ids, tenant_ids, logits, tokens, out_grad, scalars=2, plain=3,
    )
    arrived = lax.all_to_all(
        sent.reshape(n_experts, GROUP, width), "expert", 0, 0, tiled=True
    ).reshape(n_experts * GROUP, width)

    def loaded(kernel, out, *inputs, scalars=0, near=0):
        last = len(inputs) - near
        return pl.pallas_call(
            kernel,
            out_shape=out,
            in_specs=[smem()] * scalars + [anywhere()] * (last - scalars) + [vmem()] * near,
            out_specs=[vmem()] * len(out),
            scratch_shapes=[pltpu.SemaphoreType.DMA],
            compiler_params=pltpu.CompilerParams(vmem_limit_bytes=1024 * 1024),
        )(
            *inputs[:scalars],
            *[far_off(v) for v in inputs[scalars:last]],
            *[near_by(v) for v in inputs[last:]],
        )

    down_maps, up_map = loaded(
        maps_kernel,
        [held(input_down_maps.shape), held(output_up_map.shape)],
        input_down_maps, output_up_map,
    )
    keep, send = call(
        received_kernel, [held((slots, wide)), held((slots, wide))],
        where, arrived, down_maps, up_map, scalars=1,
    )
    other = swapped(send)
    unit = call(unit_kernel, held((pair, wide)), where, keep, other, scalars=1)
    line = [unit] + [turned(unit, s, 0) for s in range(1, n)]
    weights = loaded(
        weights_kernel,
        [held((n * width, hidden)), held((n * width, hidden)), held((n, hidden, width))],
        where, gate_projection_weight, up_projection_weight, down_projection_weight, unit,
        scalars=1, near=1,
    )
    crossed = [held((n, 2 * hidden, width)), held((n * width, hidden))]
    line_b = call(stack_kernel, held((2, pair, wide)), *line[2:], weights[2])
    line_a = call(stack_kernel, held((2, pair, wide)), *line[:2])
    near_a, far_b = turned(line_a, 1, 1), turned(line_b, n - 1, 1)
    near_b, far_a = turned(line_b, 1, 1), turned(line_a, n - 1, 1)
    near_a, far_b, *weights = lax.optimization_barrier((near_a, far_b, *weights))
    crossed = call(turned_weights_kernel, crossed, *weights)
    past_a, past_b = turned(near_a, 1, 1), turned(far_b, n - 1, 1)
    near_b, far_a, *crossed = lax.optimization_barrier((near_b, far_a, *crossed))
    own = [line_a, line_b, near_a, near_b, past_a, past_b, far_a, far_b]
    far = [swapped(v) for v in own]

    block = held((n, pair, wide))
    total = n * pair
    *parts, sums, token_part, grad_part, state, both_grad, gate_rows, up_rows, back_rows = call(
        expert_kernel,
        [held((n, pair, width))] * n
        + [
            held((n, pair, LANES)),
            block,
            block,
            held((total, hidden)),
            held((total, 2 * hidden)),
            held((total, columns)),
            held((total, columns)),
            held((total, columns)),
        ],
        where, *own, *far, *weights, crossed[1], input_up_maps, output_down_map,
        scalars=1,
        scratch=[
            pltpu.VMEM((total, n * width), BF),
            pltpu.VMEM((total, n * width), BF),
            pltpu.VMEM((total, LANES), F32),
            pltpu.VMEM((total, LANES), F32),
        ],
        limit=20,
    )
    keeps, theirs = {}, {}

    def reduced(j):
        keeps[j], send = call(
            functools.partial(back_kernel, j), [block, block],
            where, parts[j], both_grad, crossed[0], sums, scalars=1,
        )
        theirs[j] = swapped(send)

    def summed(j):
        return call(pair_kernel, block, keeps[j], theirs[j])

    for j in (2, 1, 3, 0):
        reduced(j)
    near = {j: turned(summed(j), n - j, 1) for j in (2, 1, 3)}
    input_up_gradient, output_down_gradient = call(
        hidden_grad_kernel,
        [shape((1, 2, columns, hidden), F32), shape((1, hidden, columns), F32)],
        state, both_grad, gate_rows, up_rows, back_rows,
    )
    tail = held((pair, width + n * LANES))
    lines = call(
        first_kernel, [tail] * n, keeps[0], theirs[0], near[1], near[2], near[3]
    )
    near = [turned(lines[j], n - j, 0) for j in range(1, n)]
    keep, send, down_rows, up_rows = call(
        last_kernel,
        [
            held((slots, width)),
            held((slots, width)),
            held((n, pair, columns)),
            held((n, pair, 2 * columns)),
        ],
        where, lines[0], *near, token_part, input_down_maps, output_up_map, scalars=1,
    )
    other = swapped(send)
    back = call(return_kernel, held((n_experts * GROUP, width)), keep, other)
    back = lax.all_to_all(
        back.reshape(n_experts, GROUP, width), "expert", 0, 0, tiled=True
    ).reshape(n_experts * GROUP, width)
    input_down_gradient, output_up_gradient = call(
        adapter_grad_kernel,
        [shape((1, width, 2 * columns), F32), shape((1, columns, width), F32)],
        token_part, grad_part, down_rows, up_rows,
    )
    mixed, input_grad = call(
        combine_kernel, [shape((n_rows, width)), shape((n_rows, width))],
        where, ids, logits, back, scalars=2,
    )
    return (
        mixed,
        input_grad,
        input_down_gradient,
        input_up_gradient,
        output_down_gradient,
        output_up_gradient,
    )


def solution(mesh):
    return jax.shard_map(
        per_device,
        mesh=mesh,
        in_specs=(
            P(("dp", "expert"), "ffn"),
            P(("dp", "expert"), "ffn"),
            P(("dp", "expert"), None),
            P(("dp", "expert")),
            P(("dp", "expert"), None),
            P("expert", None, ("dp", "ffn")),
            P("expert", None, ("dp", "ffn")),
            P("expert", ("dp", "ffn"), None),
            P("expert", "ffn", None),
            P("expert", None, None, ("dp", "ffn")),
            P("expert", ("dp", "ffn"), None),
            P("expert", None, "ffn"),
        ),
        out_specs=(
            P(("dp", "expert"), "ffn"),
            P(("dp", "expert"), "ffn"),
            P("expert", "ffn", None),
            P("expert", None, None, ("dp", "ffn")),
            P("expert", ("dp", "ffn"), None),
            P("expert", None, "ffn"),
        ),
        check_vma=False,
    )
```

```python
import functools

import jax
import jax.numpy as jnp
from jax import lax
from jax.experimental import pallas as pl
from jax.experimental.pallas import tpu as pltpu
from jax.sharding import PartitionSpec as P


RANK = 16
SCALE = 0.5
SLOTS = 3
GROUP = 8
LANES = 128
BF = jnp.bfloat16
F32 = jnp.float32
I32 = jnp.int32


def dot(left, right, dims=((1,), (0,))):
    return lax.dot_general(left, right, (dims, ((), ())), preferred_element_type=F32)


def rows_of(shape):
    return lax.broadcasted_iota(I32, shape, 0)


def lanes_of(shape):
    return lax.broadcasted_iota(I32, shape, 1)


def onehot(condition):
    return jnp.where(condition, 1.0, 0.0).astype(BF)


def two_parts(value):
    high = value.astype(BF)
    return high, (value - high.astype(F32)).astype(BF)


def vmem():
    return pl.BlockSpec(memory_space=pltpu.VMEM)


def smem():
    return pl.BlockSpec(memory_space=pltpu.SMEM)


def anywhere():
    return pl.BlockSpec(memory_space=pl.ANY)


def place_of(where):
    return where[0], where[1], where[2]


def codes_of(ids):
    n_top, n_rows = ids.shape
    chosen = [ids[k, t] for t in range(n_rows) for k in range(n_top)]
    codes = []
    for i, expert in enumerate(chosen):
        position = jnp.int32(0)
        for earlier in chosen[:i]:
            position += jnp.where(earlier == expert, 1, 0).astype(I32)
        codes.append((i // n_top, i % n_top, expert, position))
    return codes


def gates(logits):
    n_rows = logits.shape[1]
    first = jax.nn.sigmoid(logits[0:1, :] - logits[1:2, :])
    diagonal = rows_of((n_rows, n_rows)) == lanes_of((n_rows, n_rows))
    first = jnp.sum(jnp.where(diagonal, first, 0.0), axis=1, keepdims=True)
    return first, 1.0 - first


def dispatch_kernel(ids, tenants, logits, tokens, grads, out):
    n_out = out.shape[0]
    n_rows, width = tokens.shape
    main = out.shape[1] - LANES
    tail = width - main
    codes = codes_of(ids)
    first, second = gates(logits[...])
    row = rows_of((n_out, LANES))
    lane = lanes_of((n_out, LANES))
    slot, base = row % GROUP, row - row % GROUP
    head = jnp.zeros((n_out, LANES), F32)
    tails = [jnp.zeros((n_out, LANES), F32) for _ in range(SLOTS)]
    tenant_row = jnp.zeros((n_out, LANES), F32)
    for t, k, expert, position in codes:
        here = base == expert * GROUP
        as_token = lane == t
        as_grad = lane == (1 + k) * n_rows + t
        chosen = (as_token & (slot == position)) | (as_grad & (slot == SLOTS + position))
        head = jnp.where(here & chosen, 1.0, head)
        chosen = (as_token & (slot == 2 * SLOTS)) | (as_grad & (slot == 2 * SLOTS + 1))
        for p in range(SLOTS):
            tails[p] = jnp.where(here & chosen & (position == p), 1.0, tails[p])
        code = (tenants[t] + 1).astype(F32)
        tenant_row = jnp.where(
            here & (slot == 2 * SLOTS) & (lane == position), code, tenant_row
        )
    g = grads[...].astype(F32)
    source = jnp.concatenate(
        [tokens[...], (first * g).astype(BF), (second * g).astype(BF)], axis=0
    )
    n_source = 3 * n_rows
    value = dot(head[:, :n_source].astype(BF), source[:, :main])
    out[:, :main] = value.astype(BF)
    for p in range(SLOTS):
        span = slice(p * tail, (p + 1) * tail)
        value_p = dot(tails[p][:, :n_source].astype(BF), source[:, main:])
        out[:, span] = (value[:, span] + value_p).astype(BF)
    out[:, main:] = tenant_row.astype(BF)


def received_kernel(where, arrived, down_maps, up_map, keep, send):
    n_in = arrived.shape[0]
    n, width = keep.shape[0], keep.shape[1] - LANES
    main = arrived.shape[1] - LANES
    tail = width - main
    core = where[2]
    row = rows_of((n, n_in))
    column = lanes_of((n, n_in))
    start = (row // SLOTS) * GROUP
    offset = row % SLOTS
    data = arrived[...]

    def unpacked(kind):
        head = dot(onehot(column == start + kind * SLOTS + offset), data[:, :main])
        rest = sum(
            dot(
                onehot((column == start + 2 * SLOTS + kind) & (offset == p)),
                data[:, p * tail : (p + 1) * tail],
            )
            for p in range(SLOTS)
        )
        return jnp.concatenate([head.astype(BF), rest.astype(BF)], axis=1)

    tokens, grads = unpacked(0), unpacked(1)
    tenants = dot(onehot(column == start + 2 * SLOTS), data[:, main:])
    lane = lanes_of((n, LANES))
    tenant = jnp.sum(
        jnp.where(lane == rows_of((n, LANES)) % SLOTS, tenants, 0.0), axis=1, keepdims=True
    )
    mask = jnp.where((lane // RANK + 1).astype(F32) == tenant, 1.0, 0.0)
    product = dot(tokens, down_maps[0])
    back = dot(grads, up_map[0], ((1,), (1,)))
    source = rows_of((LANES, LANES)) % RANK
    target = lanes_of((LANES, LANES))

    def moved(value, offset):
        return dot(value, onehot(target - offset == source))

    gate_high, gate_low = two_parts(mask * product[:, :LANES])
    up_high, up_low = two_parts(mask * product[:, LANES:])
    back_high, back_low = two_parts(mask * back)
    token_extra = (
        moved(gate_high, 0)
        + moved(up_high, RANK)
        + moved(gate_low, 2 * RANK)
        + moved(up_low, 3 * RANK)
        + jnp.where(lane == 4 * RANK, tenant, 0.0)
    ).astype(BF)
    grad_extra = (moved(back_high, 0) + moved(back_low, RANK)).astype(BF)

    @pl.when(core == 0)
    def _():
        keep[:, :width] = tokens
        keep[:, width:] = token_extra
        send[:, :width] = grads
        send[:, width:] = grad_extra

    @pl.when(core != 0)
    def _():
        keep[:, :width] = grads
        keep[:, width:] = grad_extra
        send[:, :width] = tokens
        send[:, width:] = token_extra


def unit_kernel(where, mine, theirs, out):
    n = mine.shape[0]

    @pl.when(where[2] == 0)
    def _():
        out[:n] = mine[...]
        out[n:] = theirs[...]

    @pl.when(where[2] != 0)
    def _():
        out[:n] = theirs[...]
        out[n:] = mine[...]


def stack_kernel(first, second, *rest):
    out = rest[-1]
    out[0] = first[...]
    out[1] = second[...]


def maps_kernel(down_maps, up_map, down_maps_v, up_map_v, sem):
    copies = [
        pltpu.make_async_copy(down_maps, down_maps_v, sem),
        pltpu.make_async_copy(up_map, up_map_v, sem),
    ]
    for c in copies:
        c.start()
    for c in copies:
        c.wait()


def weights_kernel(where, gate_w, up_w, down_w, _, gate_v, up_v, down_v, sem):
    n, _, width = down_v.shape
    copy = pltpu.make_async_copy
    copies = []
    for s in range(n):
        span = pl.ds(pl.multiple_of(((where[0] - s + n) % n) * width, width), width)
        copies += [
            copy(gate_w.at[0, span, :], gate_v.at[pl.ds(s * width, width)], sem),
            copy(up_w.at[0, span, :], up_v.at[pl.ds(s * width, width)], sem),
            copy(down_w.at[0, :, span], down_v.at[s], sem),
        ]
    for c in copies:
        c.start()
    for c in copies:
        c.wait()


def turned_weights_kernel(gate_v, up_v, down_v, both_t, down_t):
    n, hidden, width = down_v.shape
    for s in range(n):
        span = slice(s * width, (s + 1) * width)
        both_t[s, :hidden] = gate_v[span].T
        both_t[s, hidden:] = up_v[span].T
        down_t[span] = down_v[s].T


def expert_kernel(where, *refs):
    n = 4
    halves = [refs[2 * k : 2 * k + 2] for k in range(2 * n)]
    own, far = halves[:n], halves[n:]
    gate_w, up_w, down_w, down_t, up_maps, out_down = refs[4 * n : 4 * n + 6]
    parts = refs[4 * n + 6 : 5 * n + 6]
    (
        sums, token_part, grad_part, hidden, both_grad, gate_rows, up_rows, back_rows,
        x_v, g_v, xe_v, ge_v,
    ) = refs[5 * n + 6 :]
    half, rows, wide = own[0][0].shape
    width = wide - LANES
    _, y, core = place_of(where)

    def fetch(tokens, grads):
        for t in range(n):
            span = slice(t * rows, (t + 1) * rows)
            of_x = [tokens[t][s // half].at[s % half] for s in range(n)]
            of_g = [grads[s][t // half].at[t % half] for s in range(n)]
            for s in range(n):
                x_v[span, s * width : (s + 1) * width] = of_x[s][:, :width]
                g_v[span, s * width : (s + 1) * width] = of_g[s][:, :width]
            xe_v[span] = sum(r[:, width:].astype(F32) for r in of_x)
            ge_v[span] = sum(r[:, width:].astype(F32) for r in of_g)
            token_part[(y - t + n) % n] = of_x[0][...]
            grad_part[(y - t + n) % n] = of_g[0][...]

    @pl.when(core == 0)
    def _():
        fetch(own, far)

    @pl.when(core != 0)
    def _():
        fetch(far, own)

    total = n * rows
    extra = xe_v[...]
    lane = lanes_of((total, LANES))
    tenant = jnp.sum(jnp.where(lane == 4 * RANK, extra, 0.0), axis=1, keepdims=True) / n
    mask = jnp.where((lane // RANK + 1).astype(F32) == tenant, 1.0, 0.0)
    row1 = rows_of((LANES, LANES))
    lane1 = lanes_of((LANES, LANES))
    spread = [onehot(row1 == lane1 % RANK + k * RANK) for k in range(2)]
    whole = (extra + pltpu.roll(extra, LANES - 2 * RANK, 1)).astype(BF)
    gate_adapter = (mask * dot(whole, spread[0])).astype(BF)
    up_adapter = (mask * dot(whole, spread[1])).astype(BF)
    extra = ge_v[...]
    whole = (extra + pltpu.roll(extra, LANES - RANK, 1)).astype(BF)
    back_adapter = (mask * dot(whole, spread[0])).astype(BF)
    gate_rows[...] = gate_adapter
    up_rows[...] = up_adapter
    back_rows[...] = back_adapter

    tokens = x_v[...]
    gate = dot(tokens, gate_w[...]) + SCALE * dot(gate_adapter, up_maps[0, 0])
    up = dot(tokens, up_w[...]) + SCALE * dot(up_adapter, up_maps[0, 1])
    sigmoid = jax.nn.sigmoid(gate)
    activated = gate * sigmoid
    state = (activated * up).astype(BF)
    hidden[...] = state
    grad_hidden = dot(g_v[...], down_t[...]) + SCALE * dot(
        back_adapter, out_down[0], ((1,), (1,))
    )
    grad_gate = (grad_hidden * up * sigmoid * (1.0 + gate * (1.0 - sigmoid))).astype(BF)
    grad_up = (grad_hidden * activated).astype(BF)
    columns = grad_gate.shape[1]
    both_grad[:, :columns] = grad_gate
    both_grad[:, columns:] = grad_up
    for s in range(n):
        result = dot(state, down_w[s]).astype(BF)
        for t in range(n):
            parts[t][s] = result[t * rows : (t + 1) * rows]

    pieces = [
        two_parts(mask * v)
        for v in (
            dot(state, out_down[0]),
            dot(grad_gate, up_maps[0, 0], ((1,), (1,))),
            dot(grad_up, up_maps[0, 1], ((1,), (1,))),
        )
    ]

    def moved(value, offset):
        return dot(value, onehot(lane1 - offset == row1 % RANK))

    value = jnp.zeros((total, LANES), F32)
    for k, (high, low) in enumerate(pieces):
        value += moved(high, k * RANK) + moved(low, (k + 3) * RANK)
    value = value.astype(BF)
    for t in range(n):
        sums[(y - t + n) % n] = value[t * rows : (t + 1) * rows]


def back_kernel(j, where, part, both_grad, both_t, sums, keep, send):
    n, rows, width = part.shape
    result = dot(both_grad[...], both_t[j]).astype(BF)

    def stored(output, gradient):
        for i in range(n):
            output[i, :, :width] = part[i]
            gradient[i, :, :width] = result[i * rows : (i + 1) * rows]
            output[i, :, width:] = sums[i]
            gradient[i, :, width:] = sums[i]

    @pl.when(where[2] == 0)
    def _():
        stored(keep, send)

    @pl.when(where[2] != 0)
    def _():
        stored(send, keep)


def hidden_grad_kernel(
    hidden, both_grad, gate_rows, up_rows, back_rows, input_up_grad, output_down_grad
):
    columns = hidden.shape[1]
    dims = ((0,), (0,))
    output_down_grad[0] = SCALE * dot(hidden[...], back_rows[...], dims)
    input_up_grad[0, 0] = SCALE * dot(gate_rows[...], both_grad[:, :columns], dims)
    input_up_grad[0, 1] = SCALE * dot(up_rows[...], both_grad[:, columns:], dims)


def joined_extra(pieces):
    value = sum(p.astype(F32) for p in pieces)
    lane = lanes_of(value.shape)
    width = 3 * RANK
    whole = value + pltpu.roll(value, LANES - width, 1)
    whole = jnp.where(lane < width, whole, 0.0)
    high, low = two_parts(whole)
    return (high.astype(F32) + pltpu.roll(low.astype(F32), width, 1)).astype(BF)


def joined(arrays):
    width = arrays[0].shape[1] - LANES
    main = sum(a[:, :width].astype(F32) for a in arrays).astype(BF)
    return main, joined_extra([a[:, width:] for a in arrays])


def pair_kernel(mine, theirs, out):
    for i in range(out.shape[0]):
        main, extra = joined([mine[i], theirs[i]])
        out[i, :, : main.shape[1]] = main
        out[i, :, main.shape[1] :] = extra


def first_kernel(mine, theirs, near1, near2, near3, *outs):
    for i, out_i in enumerate(outs):
        main, extra = joined([a[i] for a in (mine, theirs, near1, near2, near3)])
        width = main.shape[1]
        out_i[:, :width] = main
        for out in outs:
            out[:, width + i * LANES : width + (i + 1) * LANES] = extra


def tenants_of(part, width):
    extra = part[:, width:].astype(F32)
    lane = lanes_of(extra.shape)
    tenant = jnp.sum(jnp.where(lane == 4 * RANK, extra, 0.0), axis=1, keepdims=True)
    return jnp.where((lane // RANK + 1).astype(F32) == tenant, 1.0, 0.0)


def last_kernel(
    where, mine, near1, near2, near3, token_part, down_maps, up_map,
    keep, send, down_rows, up_rows,
):
    arrays = (mine, near1, near2, near3)
    n = len(arrays)
    rows, width = mine.shape[0], keep.shape[1]
    half = rows // 2
    _, y, core = place_of(where)
    row1 = rows_of((LANES, LANES))
    lane1 = lanes_of((LANES, LANES))
    spread = [onehot(row1 == lane1 % RANK + k * RANK) for k in range(3)]
    for i in range(n):
        at = width + i * LANES
        value = sum(a[:, at : at + LANES].astype(F32) for a in arrays)
        whole = (value + pltpu.roll(value, LANES - 3 * RANK, 1)).astype(BF)
        mask = tenants_of(token_part[i], width)
        down_rows[i] = (mask * dot(whole, spread[0])).astype(BF)
        up_rows[i, :, :LANES] = (mask * dot(whole, spread[1])).astype(BF)
        up_rows[i, :, LANES:] = (mask * dot(whole, spread[2])).astype(BF)
    value = sum(a[:, :width].astype(F32) for a in arrays)

    @pl.when(core == 0)
    def _():
        result = (value + SCALE * dot(down_rows[y], up_map[0])).astype(BF)
        keep[...] = result[:half]
        send[...] = result[half:]

    @pl.when(core != 0)
    def _():
        result = (value + SCALE * dot(up_rows[y], down_maps[0], ((1,), (1,)))).astype(BF)
        keep[...] = result[half:]
        send[...] = result[:half]


def adapter_grad_kernel(token_part, grad_part, down_rows, up_rows, input_down_grad, output_up_grad):
    n, _, _ = token_part.shape
    width = output_up_grad.shape[2]
    join = lambda ref, columns: jnp.concatenate([ref[i, :, :columns] for i in range(n)], axis=0)
    down = join(down_rows, LANES)
    up = join(up_rows, 2 * LANES)
    output_up_grad[0] = SCALE * dot(down, join(grad_part, width), ((0,), (0,)))
    input_down_grad[0] = SCALE * dot(join(token_part, width), up, ((0,), (0,)))


def return_kernel(mine, theirs, out):
    n_out, main = out.shape
    n, width = mine.shape
    tail = width - main
    row = rows_of((n_out, n))
    column = lanes_of((n_out, n))
    slot = row % GROUP
    base = (row // GROUP) * SLOTS
    own = onehot((slot < SLOTS) & (column == base + slot))
    other = onehot((slot >= SLOTS) & (slot < 2 * SLOTS) & (column == base + slot - SLOTS))
    value = dot(own, mine[:, :main]) + dot(other, theirs[:, :main])
    out[...] = value.astype(BF)
    for p in range(SLOTS):
        own = onehot((slot == 2 * SLOTS) & (column == base + p))
        other = onehot((slot == 2 * SLOTS + 1) & (column == base + p))
        span = slice(p * tail, (p + 1) * tail)
        rest = dot(own, mine[:, main:]) + dot(other, theirs[:, main:])
        out[:, span] = (value[:, span] + rest).astype(BF)


def combine_kernel(where, ids, logits, arrived, mixed, input_grad):
    n_in, main = arrived.shape
    n_rows, width = mixed.shape
    tail = width - main
    core = where[2]
    first, second = gates(logits[...])
    row = rows_of((n_rows, n_in))
    lane = lanes_of((n_rows, n_in))
    data = arrived[...]
    codes = codes_of(ids)

    def picked(kind, k):
        zero = jnp.zeros((n_rows, n_in), F32)
        head, tails = zero, [zero] * SLOTS
        for t, top, expert, position in codes:
            if top != k:
                continue
            base = expert * GROUP
            head = jnp.where(
                (row == t) & (lane == base + kind * SLOTS + position), 1.0, head
            )
            here = (row == t) & (lane == base + 2 * SLOTS + kind)
            for p in range(SLOTS):
                tails[p] = jnp.where(here & (position == p), 1.0, tails[p])
        rest = sum(
            dot(tails[p].astype(BF), data[:, p * tail : (p + 1) * tail]) for p in range(SLOTS)
        )
        return dot(head.astype(BF), data[:, :main]), rest

    spans = (slice(0, main), slice(main, width))
    for out, kind, one, two in (
        (mixed, core, first, second), (input_grad, 1 - core, 1.0, 1.0)
    ):
        for span, left, right in zip(spans, picked(kind, 0), picked(kind, 1)):
            out[:, span] = (one * left + two * right).astype(BF)


def shape(dims, dtype=BF):
    return jax.ShapeDtypeStruct(tuple(dims), dtype)


def held(dims, dtype=BF):
    return pltpu.VMEM(tuple(dims), dtype)


def near_by(value):
    return pltpu.with_memory_space_constraint(value, pltpu.VMEM)


def far_off(value):
    return pltpu.with_memory_space_constraint(value, pltpu.HBM)


def per_device(
    tokens,
    out_grad,
    expert_ids,
    tenant_ids,
    router_logits,
    gate_projection_weight,
    up_projection_weight,
    down_projection_weight,
    input_down_maps,
    input_up_maps,
    output_down_map,
    output_up_map,
):
    n_experts = lax.axis_size("expert")
    n_data = lax.axis_size("dp")
    n = lax.axis_size("ffn")
    n_rows, width = tokens.shape
    hidden = gate_projection_weight.shape[2]
    columns = output_down_map.shape[2]
    slots = SLOTS * n_experts
    pair = 2 * slots
    wide = width + LANES
    plane = ("dp", "ffn")
    data_index = lax.axis_index("dp")
    where = jnp.stack([lax.axis_index("ffn"), data_index // 2, data_index % 2]).astype(I32)

    def turn(distance, stage):
        pairs = []
        for chip in range(n):
            for core in range(2):
                for split in range(n):
                    if core == stage:
                        to = (chip, (split + distance) % n)
                    else:
                        to = ((chip + distance) % n, split)
                    pairs.append(
                        ((2 * chip + core) * n + split, (2 * to[0] + core) * n + to[1])
                    )
        return pairs

    def turned(value, distance, stage):
        return lax.ppermute(value, plane, turn(distance, stage))

    def swapped(value):
        return lax.ppermute(value, "dp", [(i, i ^ 1) for i in range(n_data)])

    def call(kernel, out, *inputs, scalars=0, plain=0, scratch=(), limit=8):
        several = isinstance(out, list)
        return pl.pallas_call(
            kernel,
            out_shape=out,
            in_specs=[smem()] * scalars + [vmem()] * (len(inputs) - scalars),
            out_specs=[vmem()] * len(out) if several else vmem(),
            scratch_shapes=scratch,
            compiler_params=pltpu.CompilerParams(vmem_limit_bytes=limit * 1024 * 1024),
        )(*[far_off(v) if plain else v for v in inputs[: scalars + plain]], *[near_by(v) for v in inputs[scalars + plain :]])

    ids, logits = expert_ids.T, router_logits.T
    main = width * 2 * SLOTS // GROUP
    sent = call(
        dispatch_kernel, held((n_experts * GROUP, main + LANES)),
        ids, tenant_ids, logits, tokens, out_grad, scalars=2, plain=3,
    )
    arrived = lax.all_to_all(
        sent.reshape(n_experts, GROUP, main + LANES), "expert", 0, 0, tiled=True
    ).reshape(n_experts * GROUP, main + LANES)

    def loaded(kernel, out, *inputs, scalars=0, near=0):
        last = len(inputs) - near
        return pl.pallas_call(
            kernel,
            out_shape=out,
            in_specs=[smem()] * scalars + [anywhere()] * (last - scalars) + [vmem()] * near,
            out_specs=[vmem()] * len(out),
            scratch_shapes=[pltpu.SemaphoreType.DMA],
            compiler_params=pltpu.CompilerParams(vmem_limit_bytes=1024 * 1024),
        )(
            *inputs[:scalars],
            *[far_off(v) for v in inputs[scalars:last]],
            *[near_by(v) for v in inputs[last:]],
        )

    down_maps, up_map = loaded(
        maps_kernel,
        [held(input_down_maps.shape), held(output_up_map.shape)],
        input_down_maps, output_up_map,
    )
    keep, send = call(
        received_kernel, [held((slots, wide)), held((slots, wide))],
        where, arrived, down_maps, up_map, scalars=1,
    )
    other = swapped(send)
    unit = call(unit_kernel, held((pair, wide)), where, keep, other, scalars=1)
    line = [unit] + [turned(unit, s, 0) for s in range(1, n)]
    weights = loaded(
        weights_kernel,
        [held((n * width, hidden)), held((n * width, hidden)), held((n, hidden, width))],
        where, gate_projection_weight, up_projection_weight, down_projection_weight, unit,
        scalars=1, near=1,
    )
    crossed = [held((n, 2 * hidden, width)), held((n * width, hidden))]
    line_b = call(stack_kernel, held((2, pair, wide)), *line[2:], weights[2])
    line_a = call(stack_kernel, held((2, pair, wide)), *line[:2])
    near_a, far_b = turned(line_a, 1, 1), turned(line_b, n - 1, 1)
    near_b, far_a = turned(line_b, 1, 1), turned(line_a, n - 1, 1)
    near_a, far_b, *weights = lax.optimization_barrier((near_a, far_b, *weights))
    crossed = call(turned_weights_kernel, crossed, *weights)
    past_a, past_b = turned(near_a, 1, 1), turned(far_b, n - 1, 1)
    near_b, far_a, *crossed = lax.optimization_barrier((near_b, far_a, *crossed))
    own = [line_a, line_b, near_a, near_b, past_a, past_b, far_a, far_b]
    far = [swapped(v) for v in own]

    block = held((n, pair, wide))
    total = n * pair
    *parts, sums, token_part, grad_part, state, both_grad, gate_rows, up_rows, back_rows = call(
        expert_kernel,
        [held((n, pair, width))] * n
        + [
            held((n, pair, LANES)),
            block,
            block,
            held((total, hidden)),
            held((total, 2 * hidden)),
            held((total, columns)),
            held((total, columns)),
            held((total, columns)),
        ],
        where, *own, *far, *weights, crossed[1], input_up_maps, output_down_map,
        scalars=1,
        scratch=[
            pltpu.VMEM((total, n * width), BF),
            pltpu.VMEM((total, n * width), BF),
            pltpu.VMEM((total, LANES), F32),
            pltpu.VMEM((total, LANES), F32),
        ],
        limit=20,
    )
    keeps, theirs = {}, {}

    def reduced(j):
        keeps[j], send = call(
            functools.partial(back_kernel, j), [block, block],
            where, parts[j], both_grad, crossed[0], sums, scalars=1,
        )
        theirs[j] = swapped(send)

    def summed(j):
        return call(pair_kernel, block, keeps[j], theirs[j])

    for j in (2, 1, 3, 0):
        reduced(j)
    near = {j: turned(summed(j), n - j, 1) for j in (2, 1, 3)}
    input_up_gradient, output_down_gradient = call(
        hidden_grad_kernel,
        [shape((1, 2, columns, hidden), F32), shape((1, hidden, columns), F32)],
        state, both_grad, gate_rows, up_rows, back_rows,
    )
    tail = held((pair, width + n * LANES))
    lines = call(
        first_kernel, [tail] * n, keeps[0], theirs[0], near[1], near[2], near[3]
    )
    near = [turned(lines[j], n - j, 0) for j in range(1, n)]
    keep, send, down_rows, up_rows = call(
        last_kernel,
        [
            held((slots, width)),
            held((slots, width)),
            held((n, pair, columns)),
            held((n, pair, 2 * columns)),
        ],
        where, lines[0], *near, token_part, input_down_maps, output_up_map, scalars=1,
    )
    other = swapped(send)
    back = call(return_kernel, held((n_experts * GROUP, main)), keep, other)
    back = lax.all_to_all(
        back.reshape(n_experts, GROUP, main), "expert", 0, 0, tiled=True
    ).reshape(n_experts * GROUP, main)
    input_down_gradient, output_up_gradient = call(
        adapter_grad_kernel,
        [shape((1, width, 2 * columns), F32), shape((1, columns, width), F32)],
        token_part, grad_part, down_rows, up_rows,
    )
    mixed, input_grad = call(
        combine_kernel, [shape((n_rows, width)), shape((n_rows, width))],
        where, ids, logits, back, scalars=2,
    )
    return (
        mixed,
        input_grad,
        input_down_gradient,
        input_up_gradient,
        output_down_gradient,
        output_up_gradient,
    )


def solution(mesh):
    return jax.shard_map(
        per_device,
        mesh=mesh,
        in_specs=(
            P(("dp", "expert"), "ffn"),
            P(("dp", "expert"), "ffn"),
            P(("dp", "expert"), None),
            P(("dp", "expert")),
            P(("dp", "expert"), None),
            P("expert", None, ("dp", "ffn")),
            P("expert", None, ("dp", "ffn")),
            P("expert", ("dp", "ffn"), None),
            P("expert", "ffn", None),
            P("expert", None, None, ("dp", "ffn")),
            P("expert", ("dp", "ffn"), None),
            P("expert", None, "ffn"),
        ),
        out_specs=(
            P(("dp", "expert"), "ffn"),
            P(("dp", "expert"), "ffn"),
            P("expert", "ffn", None),
            P("expert", None, None, ("dp", "ffn")),
            P("expert", ("dp", "ffn"), None),
            P("expert", None, "ffn"),
        ),
        check_vma=False,
    )
```

```python
import functools

import jax
import jax.numpy as jnp
from jax import lax
from jax.experimental import pallas as pl
from jax.experimental.pallas import tpu as pltpu
from jax.sharding import PartitionSpec as P


RANK = 16
SCALE = 0.5
SLOTS = 3
GROUP = 8
LANES = 128
BF = jnp.bfloat16
F32 = jnp.float32
I32 = jnp.int32


def dot(left, right, dims=((1,), (0,))):
    return lax.dot_general(left, right, (dims, ((), ())), preferred_element_type=F32)


def rows_of(shape):
    return lax.broadcasted_iota(I32, shape, 0)


def lanes_of(shape):
    return lax.broadcasted_iota(I32, shape, 1)


def onehot(condition):
    return jnp.where(condition, 1.0, 0.0).astype(BF)


def two_parts(value):
    high = value.astype(BF)
    return high, (value - high.astype(F32)).astype(BF)


def vmem():
    return pl.BlockSpec(memory_space=pltpu.VMEM)


def smem():
    return pl.BlockSpec(memory_space=pltpu.SMEM)


def anywhere():
    return pl.BlockSpec(memory_space=pl.ANY)


def place_of(where):
    return where[0], where[1], where[2]


def codes_of(ids):
    n_top, n_rows = ids.shape
    chosen = [ids[k, t] for t in range(n_rows) for k in range(n_top)]
    codes = []
    for i, expert in enumerate(chosen):
        position = jnp.int32(0)
        for earlier in chosen[:i]:
            position += jnp.where(earlier == expert, 1, 0).astype(I32)
        codes.append((i // n_top, i % n_top, expert, position))
    return codes


def gates(logits):
    n_rows = logits.shape[1]
    first = jax.nn.sigmoid(logits[0:1, :] - logits[1:2, :])
    diagonal = rows_of((n_rows, n_rows)) == lanes_of((n_rows, n_rows))
    first = jnp.sum(jnp.where(diagonal, first, 0.0), axis=1, keepdims=True)
    return first, 1.0 - first


def dispatch_kernel(ids, tenants, logits, tokens, grads, out):
    n_out = out.shape[0]
    n_rows, width = tokens.shape
    main = out.shape[1] - LANES
    tail = width - main
    codes = codes_of(ids)
    first, second = gates(logits[...])
    row = rows_of((n_out, LANES))
    lane = lanes_of((n_out, LANES))
    slot, base = row % GROUP, row - row % GROUP
    head = jnp.zeros((n_out, LANES), F32)
    tails = [jnp.zeros((n_out, LANES), F32) for _ in range(SLOTS)]
    tenant_row = jnp.zeros((n_out, LANES), F32)
    for t, k, expert, position in codes:
        here = base == expert * GROUP
        as_token = lane == t
        as_grad = lane == (1 + k) * n_rows + t
        chosen = (as_token & (slot == position)) | (as_grad & (slot == SLOTS + position))
        head = jnp.where(here & chosen, 1.0, head)
        chosen = (as_token & (slot == 2 * SLOTS)) | (as_grad & (slot == 2 * SLOTS + 1))
        for p in range(SLOTS):
            tails[p] = jnp.where(here & chosen & (position == p), 1.0, tails[p])
        code = (tenants[t] + 1).astype(F32)
        tenant_row = jnp.where(
            here & (slot == 2 * SLOTS) & (lane == position), code, tenant_row
        )
    g = grads[...].astype(F32)
    source = jnp.concatenate(
        [tokens[...], (first * g).astype(BF), (second * g).astype(BF)], axis=0
    )
    n_source = 3 * n_rows
    value = dot(head[:, :n_source].astype(BF), source[:, :main])
    out[:, :main] = value.astype(BF)
    for p in range(SLOTS):
        span = slice(p * tail, (p + 1) * tail)
        value_p = dot(tails[p][:, :n_source].astype(BF), source[:, main:])
        out[:, span] = (value[:, span] + value_p).astype(BF)
    out[:, main:] = tenant_row.astype(BF)


def received_kernel(where, arrived, down_maps, up_map, keep, send):
    n_in = arrived.shape[0]
    n, width = keep.shape[0], keep.shape[1] - LANES
    main = arrived.shape[1] - LANES
    tail = width - main
    core = where[2]
    row = rows_of((n, n_in))
    column = lanes_of((n, n_in))
    start = (row // SLOTS) * GROUP
    offset = row % SLOTS
    data = arrived[...]

    def unpacked(kind):
        head = dot(onehot(column == start + kind * SLOTS + offset), data[:, :main])
        rest = sum(
            dot(
                onehot((column == start + 2 * SLOTS + kind) & (offset == p)),
                data[:, p * tail : (p + 1) * tail],
            )
            for p in range(SLOTS)
        )
        return jnp.concatenate([head.astype(BF), rest.astype(BF)], axis=1)

    tokens, grads = unpacked(0), unpacked(1)
    tenants = dot(onehot(column == start + 2 * SLOTS), data[:, main:])
    lane = lanes_of((n, LANES))
    tenant = jnp.sum(
        jnp.where(lane == rows_of((n, LANES)) % SLOTS, tenants, 0.0), axis=1, keepdims=True
    )
    mask = jnp.where((lane // RANK + 1).astype(F32) == tenant, 1.0, 0.0)
    product = dot(tokens, down_maps[0])
    back = dot(grads, up_map[0], ((1,), (1,)))
    source = rows_of((LANES, LANES)) % RANK
    target = lanes_of((LANES, LANES))

    def moved(value, offset):
        return dot(value, onehot(target - offset == source))

    gate_high, gate_low = two_parts(mask * product[:, :LANES])
    up_high, up_low = two_parts(mask * product[:, LANES:])
    back_high, back_low = two_parts(mask * back)
    token_extra = (
        moved(gate_high, 0)
        + moved(up_high, RANK)
        + moved(gate_low, 2 * RANK)
        + moved(up_low, 3 * RANK)
        + jnp.where(lane == 4 * RANK, tenant, 0.0)
    ).astype(BF)
    grad_extra = (moved(back_high, 0) + moved(back_low, RANK)).astype(BF)

    @pl.when(core == 0)
    def _():
        keep[:, :width] = tokens
        keep[:, width:] = token_extra
        send[:, :width] = grads
        send[:, width:] = grad_extra

    @pl.when(core != 0)
    def _():
        keep[:, :width] = grads
        keep[:, width:] = grad_extra
        send[:, :width] = tokens
        send[:, width:] = token_extra


def unit_kernel(where, mine, theirs, out):
    n = mine.shape[0]

    @pl.when(where[2] == 0)
    def _():
        out[:n] = mine[...]
        out[n:] = theirs[...]

    @pl.when(where[2] != 0)
    def _():
        out[:n] = theirs[...]
        out[n:] = mine[...]


def stack_kernel(first, second, out):
    out[0] = first[...]
    out[1] = second[...]


def maps_kernel(down_maps, up_map, down_maps_v, up_map_v, sem):
    copies = [
        pltpu.make_async_copy(down_maps, down_maps_v, sem),
        pltpu.make_async_copy(up_map, up_map_v, sem),
    ]
    for c in copies:
        c.start()
    for c in copies:
        c.wait()


def weights_kernel(where, gate_w, up_w, down_w, _, gate_v, up_v, down_v, sem):
    n, _, width = down_v.shape
    copy = pltpu.make_async_copy
    copies = []
    for s in range(n):
        span = pl.ds(pl.multiple_of(((where[0] - s + n) % n) * width, width), width)
        copies += [
            copy(gate_w.at[0, span, :], gate_v.at[pl.ds(s * width, width)], sem),
            copy(up_w.at[0, span, :], up_v.at[pl.ds(s * width, width)], sem),
            copy(down_w.at[0, :, span], down_v.at[s], sem),
        ]
    for c in copies:
        c.start()
    for c in copies:
        c.wait()


def turned_weights_kernel(gate_v, up_v, down_v, both_t, down_t):
    n, hidden, width = down_v.shape
    for s in range(n):
        span = slice(s * width, (s + 1) * width)
        both_t[s, :hidden] = gate_v[span].T
        both_t[s, hidden:] = up_v[span].T
        down_t[span] = down_v[s].T


def expert_kernel(where, *refs):
    n = 4
    halves = [refs[2 * k : 2 * k + 2] for k in range(2 * n)]
    own, far = halves[:n], halves[n:]
    gate_w, up_w, down_w, down_t, up_maps, out_down = refs[4 * n : 4 * n + 6]
    parts = refs[4 * n + 6 : 5 * n + 6]
    (
        sums, token_part, grad_part, hidden, both_grad, gate_rows, up_rows, back_rows,
        x_v, g_v, xe_v, ge_v,
    ) = refs[5 * n + 6 :]
    half, rows, wide = own[0][0].shape
    width = wide - LANES
    _, y, core = place_of(where)

    def fetch(tokens, grads):
        for t in range(n):
            span = slice(t * rows, (t + 1) * rows)
            of_x = [tokens[t][s // half].at[s % half] for s in range(n)]
            of_g = [grads[s][t // half].at[t % half] for s in range(n)]
            for s in range(n):
                x_v[span, s * width : (s + 1) * width] = of_x[s][:, :width]
                g_v[span, s * width : (s + 1) * width] = of_g[s][:, :width]
            xe_v[span] = sum(r[:, width:].astype(F32) for r in of_x)
            ge_v[span] = sum(r[:, width:].astype(F32) for r in of_g)
            token_part[(y - t + n) % n] = of_x[0][...]
            grad_part[(y - t + n) % n] = of_g[0][...]

    @pl.when(core == 0)
    def _():
        fetch(own, far)

    @pl.when(core != 0)
    def _():
        fetch(far, own)

    total = n * rows
    extra = xe_v[...]
    lane = lanes_of((total, LANES))
    tenant = jnp.sum(jnp.where(lane == 4 * RANK, extra, 0.0), axis=1, keepdims=True) / n
    mask = jnp.where((lane // RANK + 1).astype(F32) == tenant, 1.0, 0.0)
    row1 = rows_of((LANES, LANES))
    lane1 = lanes_of((LANES, LANES))
    spread = [onehot(row1 == lane1 % RANK + k * RANK) for k in range(2)]
    whole = (extra + pltpu.roll(extra, LANES - 2 * RANK, 1)).astype(BF)
    gate_adapter = (mask * dot(whole, spread[0])).astype(BF)
    up_adapter = (mask * dot(whole, spread[1])).astype(BF)
    extra = ge_v[...]
    whole = (extra + pltpu.roll(extra, LANES - RANK, 1)).astype(BF)
    back_adapter = (mask * dot(whole, spread[0])).astype(BF)
    gate_rows[...] = gate_adapter
    up_rows[...] = up_adapter
    back_rows[...] = back_adapter

    tokens = x_v[...]
    gate = dot(tokens, gate_w[...]) + SCALE * dot(gate_adapter, up_maps[0, 0])
    up = dot(tokens, up_w[...]) + SCALE * dot(up_adapter, up_maps[0, 1])
    sigmoid = jax.nn.sigmoid(gate)
    activated = gate * sigmoid
    state = (activated * up).astype(BF)
    hidden[...] = state
    grad_hidden = dot(g_v[...], down_t[...]) + SCALE * dot(
        back_adapter, out_down[0], ((1,), (1,))
    )
    grad_gate = (grad_hidden * up * sigmoid * (1.0 + gate * (1.0 - sigmoid))).astype(BF)
    grad_up = (grad_hidden * activated).astype(BF)
    columns = grad_gate.shape[1]
    both_grad[:, :columns] = grad_gate
    both_grad[:, columns:] = grad_up
    for s in range(n):
        result = dot(state, down_w[s]).astype(BF)
        for t in range(n):
            parts[t][s] = result[t * rows : (t + 1) * rows]

    pieces = [
        two_parts(mask * v)
        for v in (
            dot(state, out_down[0]),
            dot(grad_gate, up_maps[0, 0], ((1,), (1,))),
            dot(grad_up, up_maps[0, 1], ((1,), (1,))),
        )
    ]

    def moved(value, offset):
        return dot(value, onehot(lane1 - offset == row1 % RANK))

    value = jnp.zeros((total, LANES), F32)
    for k, (high, low) in enumerate(pieces):
        value += moved(high, k * RANK) + moved(low, (k + 3) * RANK)
    value = value.astype(BF)
    for t in range(n):
        sums[(y - t + n) % n] = value[t * rows : (t + 1) * rows]


def back_kernel(j, where, part, both_grad, both_t, sums, keep, send):
    n, rows, width = part.shape
    result = dot(both_grad[...], both_t[j]).astype(BF)

    def stored(output, gradient):
        for i in range(n):
            output[i, :, :width] = part[i]
            gradient[i, :, :width] = result[i * rows : (i + 1) * rows]
            output[i, :, width:] = sums[i]
            gradient[i, :, width:] = sums[i]

    @pl.when(where[2] == 0)
    def _():
        stored(keep, send)

    @pl.when(where[2] != 0)
    def _():
        stored(send, keep)


def hidden_grad_kernel(
    hidden, both_grad, gate_rows, up_rows, back_rows, input_up_grad, output_down_grad
):
    columns = hidden.shape[1]
    dims = ((0,), (0,))
    output_down_grad[0] = SCALE * dot(hidden[...], back_rows[...], dims)
    input_up_grad[0, 0] = SCALE * dot(gate_rows[...], both_grad[:, :columns], dims)
    input_up_grad[0, 1] = SCALE * dot(up_rows[...], both_grad[:, columns:], dims)


def joined_extra(pieces):
    value = sum(p.astype(F32) for p in pieces)
    lane = lanes_of(value.shape)
    width = 3 * RANK
    whole = value + pltpu.roll(value, LANES - width, 1)
    whole = jnp.where(lane < width, whole, 0.0)
    high, low = two_parts(whole)
    return (high.astype(F32) + pltpu.roll(low.astype(F32), width, 1)).astype(BF)


def joined(arrays):
    width = arrays[0].shape[1] - LANES
    main = sum(a[:, :width].astype(F32) for a in arrays).astype(BF)
    return main, joined_extra([a[:, width:] for a in arrays])


def pair_kernel(mine, theirs, out):
    for i in range(out.shape[0]):
        main, extra = joined([mine[i], theirs[i]])
        out[i, :, : main.shape[1]] = main
        out[i, :, main.shape[1] :] = extra


def first_kernel(mine, theirs, near1, near2, near3, *outs):
    for i, out_i in enumerate(outs):
        main, extra = joined([a[i] for a in (mine, theirs, near1, near2, near3)])
        width = main.shape[1]
        out_i[:, :width] = main
        for out in outs:
            out[:, width + i * LANES : width + (i + 1) * LANES] = extra


def tenants_of(part, width):
    extra = part[:, width:].astype(F32)
    lane = lanes_of(extra.shape)
    tenant = jnp.sum(jnp.where(lane == 4 * RANK, extra, 0.0), axis=1, keepdims=True)
    return jnp.where((lane // RANK + 1).astype(F32) == tenant, 1.0, 0.0)


def last_kernel(
    where, mine, near1, near2, near3, token_part, down_maps, up_map,
    keep, send, down_rows, up_rows,
):
    arrays = (mine, near1, near2, near3)
    n = len(arrays)
    rows, width = mine.shape[0], keep.shape[1]
    half = rows // 2
    _, y, core = place_of(where)
    row1 = rows_of((LANES, LANES))
    lane1 = lanes_of((LANES, LANES))
    spread = [onehot(row1 == lane1 % RANK + k * RANK) for k in range(3)]
    for i in range(n):
        at = width + i * LANES
        value = sum(a[:, at : at + LANES].astype(F32) for a in arrays)
        whole = (value + pltpu.roll(value, LANES - 3 * RANK, 1)).astype(BF)
        mask = tenants_of(token_part[i], width)
        down_rows[i] = (mask * dot(whole, spread[0])).astype(BF)
        up_rows[i, :, :LANES] = (mask * dot(whole, spread[1])).astype(BF)
        up_rows[i, :, LANES:] = (mask * dot(whole, spread[2])).astype(BF)
    value = sum(a[:, :width].astype(F32) for a in arrays)

    @pl.when(core == 0)
    def _():
        result = (value + SCALE * dot(down_rows[y], up_map[0])).astype(BF)
        keep[...] = result[:half]
        send[...] = result[half:]

    @pl.when(core != 0)
    def _():
        result = (value + SCALE * dot(up_rows[y], down_maps[0], ((1,), (1,)))).astype(BF)
        keep[...] = result[half:]
        send[...] = result[:half]


def adapter_grad_kernel(token_part, grad_part, down_rows, up_rows, input_down_grad, output_up_grad):
    n, _, _ = token_part.shape
    width = output_up_grad.shape[2]
    join = lambda ref, columns: jnp.concatenate([ref[i, :, :columns] for i in range(n)], axis=0)
    down = join(down_rows, LANES)
    up = join(up_rows, 2 * LANES)
    output_up_grad[0] = SCALE * dot(down, join(grad_part, width), ((0,), (0,)))
    input_down_grad[0] = SCALE * dot(join(token_part, width), up, ((0,), (0,)))


def return_kernel(mine, theirs, out):
    n_out, main = out.shape
    n, width = mine.shape
    tail = width - main
    row = rows_of((n_out, n))
    column = lanes_of((n_out, n))
    slot = row % GROUP
    base = (row // GROUP) * SLOTS
    own = onehot((slot < SLOTS) & (column == base + slot))
    other = onehot((slot >= SLOTS) & (slot < 2 * SLOTS) & (column == base + slot - SLOTS))
    value = dot(own, mine[:, :main]) + dot(other, theirs[:, :main])
    out[...] = value.astype(BF)
    for p in range(SLOTS):
        own = onehot((slot == 2 * SLOTS) & (column == base + p))
        other = onehot((slot == 2 * SLOTS + 1) & (column == base + p))
        span = slice(p * tail, (p + 1) * tail)
        rest = dot(own, mine[:, main:]) + dot(other, theirs[:, main:])
        out[:, span] = (value[:, span] + rest).astype(BF)


def combine_kernel(where, ids, logits, arrived, mixed, input_grad):
    n_in, main = arrived.shape
    n_rows, width = mixed.shape
    tail = width - main
    core = where[2]
    first, second = gates(logits[...])
    row = rows_of((n_rows, n_in))
    lane = lanes_of((n_rows, n_in))
    data = arrived[...]
    codes = codes_of(ids)

    def picked(kind, k):
        zero = jnp.zeros((n_rows, n_in), F32)
        head, tails = zero, [zero] * SLOTS
        for t, top, expert, position in codes:
            if top != k:
                continue
            base = expert * GROUP
            head = jnp.where(
                (row == t) & (lane == base + kind * SLOTS + position), 1.0, head
            )
            here = (row == t) & (lane == base + 2 * SLOTS + kind)
            for p in range(SLOTS):
                tails[p] = jnp.where(here & (position == p), 1.0, tails[p])
        rest = sum(
            dot(tails[p].astype(BF), data[:, p * tail : (p + 1) * tail]) for p in range(SLOTS)
        )
        return dot(head.astype(BF), data[:, :main]), rest

    spans = (slice(0, main), slice(main, width))
    for out, kind, one, two in (
        (mixed, core, first, second), (input_grad, 1 - core, 1.0, 1.0)
    ):
        for span, left, right in zip(spans, picked(kind, 0), picked(kind, 1)):
            out[:, span] = (one * left + two * right).astype(BF)


def shape(dims, dtype=BF):
    return jax.ShapeDtypeStruct(tuple(dims), dtype)


def held(dims, dtype=BF):
    return pltpu.VMEM(tuple(dims), dtype)


def near_by(value):
    return pltpu.with_memory_space_constraint(value, pltpu.VMEM)


def far_off(value):
    return pltpu.with_memory_space_constraint(value, pltpu.HBM)


def per_device(
    tokens,
    out_grad,
    expert_ids,
    tenant_ids,
    router_logits,
    gate_projection_weight,
    up_projection_weight,
    down_projection_weight,
    input_down_maps,
    input_up_maps,
    output_down_map,
    output_up_map,
):
    n_experts = lax.axis_size("expert")
    n_data = lax.axis_size("dp")
    n = lax.axis_size("ffn")
    n_rows, width = tokens.shape
    hidden = gate_projection_weight.shape[2]
    columns = output_down_map.shape[2]
    slots = SLOTS * n_experts
    pair = 2 * slots
    wide = width + LANES
    plane = ("dp", "ffn")
    data_index = lax.axis_index("dp")
    where = jnp.stack([lax.axis_index("ffn"), data_index // 2, data_index % 2]).astype(I32)

    def turn(distance, stage):
        pairs = []
        for chip in range(n):
            for core in range(2):
                for split in range(n):
                    if core == stage:
                        to = (chip, (split + distance) % n)
                    else:
                        to = ((chip + distance) % n, split)
                    pairs.append(
                        ((2 * chip + core) * n + split, (2 * to[0] + core) * n + to[1])
                    )
        return pairs

    def turned(value, distance, stage):
        return lax.ppermute(value, plane, turn(distance, stage))

    def swapped(value):
        return lax.ppermute(value, "dp", [(i, i ^ 1) for i in range(n_data)])

    def call(kernel, out, *inputs, scalars=0, plain=0, scratch=(), limit=8):
        several = isinstance(out, list)
        return pl.pallas_call(
            kernel,
            out_shape=out,
            in_specs=[smem()] * scalars + [vmem()] * (len(inputs) - scalars),
            out_specs=[vmem()] * len(out) if several else vmem(),
            scratch_shapes=scratch,
            compiler_params=pltpu.CompilerParams(vmem_limit_bytes=limit * 1024 * 1024),
        )(*[far_off(v) if plain else v for v in inputs[: scalars + plain]], *[near_by(v) for v in inputs[scalars + plain :]])

    ids, logits = expert_ids.T, router_logits.T
    main = width * 2 * SLOTS // GROUP
    sent = call(
        dispatch_kernel, held((n_experts * GROUP, main + LANES)),
        ids, tenant_ids, logits, tokens, out_grad, scalars=2, plain=3,
    )
    arrived = lax.all_to_all(
        sent.reshape(n_experts, GROUP, main + LANES), "expert", 0, 0, tiled=True
    ).reshape(n_experts * GROUP, main + LANES)

    def loaded(kernel, out, *inputs, scalars=0, near=0):
        last = len(inputs) - near
        return pl.pallas_call(
            kernel,
            out_shape=out,
            in_specs=[smem()] * scalars + [anywhere()] * (last - scalars) + [vmem()] * near,
            out_specs=[vmem()] * len(out),
            scratch_shapes=[pltpu.SemaphoreType.DMA],
            compiler_params=pltpu.CompilerParams(vmem_limit_bytes=1024 * 1024),
        )(
            *inputs[:scalars],
            *[far_off(v) for v in inputs[scalars:last]],
            *[near_by(v) for v in inputs[last:]],
        )

    down_maps, up_map = loaded(
        maps_kernel,
        [held(input_down_maps.shape), held(output_up_map.shape)],
        input_down_maps, output_up_map,
    )
    keep, send = call(
        received_kernel, [held((slots, wide)), held((slots, wide))],
        where, arrived, down_maps, up_map, scalars=1,
    )
    other = swapped(send)
    unit = call(unit_kernel, held((pair, wide)), where, keep, other, scalars=1)
    line = [unit] + [turned(unit, s, 0) for s in range(1, n)]
    weights = loaded(
        weights_kernel,
        [held((n * width, hidden)), held((n * width, hidden)), held((n, hidden, width))],
        where, gate_projection_weight, up_projection_weight, down_projection_weight, unit,
        scalars=1, near=1,
    )
    crossed = [held((n, 2 * hidden, width)), held((n * width, hidden))]
    line_b = call(stack_kernel, held((2, pair, wide)), *line[2:])
    line_a = call(stack_kernel, held((2, pair, wide)), *line[:2])
    near_a, far_b = turned(line_a, 1, 1), turned(line_b, n - 1, 1)
    near_b, far_a = turned(line_b, 1, 1), turned(line_a, n - 1, 1)
    near_a, far_b, *weights = lax.optimization_barrier((near_a, far_b, *weights))
    crossed = call(turned_weights_kernel, crossed, *weights)
    past_a, past_b = turned(near_a, 1, 1), turned(far_b, n - 1, 1)
    near_b, far_a, *crossed = lax.optimization_barrier((near_b, far_a, *crossed))
    own = [line_a, line_b, near_a, near_b, past_a, past_b, far_a, far_b]
    far = [swapped(v) for v in own]

    block = held((n, pair, wide))
    total = n * pair
    *parts, sums, token_part, grad_part, state, both_grad, gate_rows, up_rows, back_rows = call(
        expert_kernel,
        [held((n, pair, width))] * n
        + [
            held((n, pair, LANES)),
            block,
            block,
            held((total, hidden)),
            held((total, 2 * hidden)),
            held((total, columns)),
            held((total, columns)),
            held((total, columns)),
        ],
        where, *own, *far, *weights, crossed[1], input_up_maps, output_down_map,
        scalars=1,
        scratch=[
            pltpu.VMEM((total, n * width), BF),
            pltpu.VMEM((total, n * width), BF),
            pltpu.VMEM((total, LANES), F32),
            pltpu.VMEM((total, LANES), F32),
        ],
        limit=20,
    )
    keeps, theirs = {}, {}

    def reduced(j):
        keeps[j], send = call(
            functools.partial(back_kernel, j), [block, block],
            where, parts[j], both_grad, crossed[0], sums, scalars=1,
        )
        theirs[j] = swapped(send)

    def summed(j):
        return call(pair_kernel, block, keeps[j], theirs[j])

    for j in (2, 1, 3, 0):
        reduced(j)
    near = {j: turned(summed(j), n - j, 1) for j in (2, 1, 3)}
    input_up_gradient, output_down_gradient = call(
        hidden_grad_kernel,
        [shape((1, 2, columns, hidden), F32), shape((1, hidden, columns), F32)],
        state, both_grad, gate_rows, up_rows, back_rows,
    )
    tail = held((pair, width + n * LANES))
    lines = call(
        first_kernel, [tail] * n, keeps[0], theirs[0], near[1], near[2], near[3]
    )
    near = [turned(lines[j], n - j, 0) for j in range(1, n)]
    keep, send, down_rows, up_rows = call(
        last_kernel,
        [
            held((slots, width)),
            held((slots, width)),
            held((n, pair, columns)),
            held((n, pair, 2 * columns)),
        ],
        where, lines[0], *near, token_part, input_down_maps, output_up_map, scalars=1,
    )
    other = swapped(send)
    back = call(return_kernel, held((n_experts * GROUP, main)), keep, other)
    back = lax.all_to_all(
        back.reshape(n_experts, GROUP, main), "expert", 0, 0, tiled=True
    ).reshape(n_experts * GROUP, main)
    input_down_gradient, output_up_gradient = call(
        adapter_grad_kernel,
        [shape((1, width, 2 * columns), F32), shape((1, columns, width), F32)],
        token_part, grad_part, down_rows, up_rows,
    )
    mixed, input_grad = call(
        combine_kernel, [shape((n_rows, width)), shape((n_rows, width))],
        where, ids, logits, back, scalars=2,
    )
    return (
        mixed,
        input_grad,
        input_down_gradient,
        input_up_gradient,
        output_down_gradient,
        output_up_gradient,
    )


def solution(mesh):
    return jax.shard_map(
        per_device,
        mesh=mesh,
        in_specs=(
            P(("dp", "expert"), "ffn"),
            P(("dp", "expert"), "ffn"),
            P(("dp", "expert"), None),
            P(("dp", "expert")),
            P(("dp", "expert"), None),
            P("expert", None, ("dp", "ffn")),
            P("expert", None, ("dp", "ffn")),
            P("expert", ("dp", "ffn"), None),
            P("expert", "ffn", None),
            P("expert", None, None, ("dp", "ffn")),
            P("expert", ("dp", "ffn"), None),
            P("expert", None, "ffn"),
        ),
        out_specs=(
            P(("dp", "expert"), "ffn"),
            P(("dp", "expert"), "ffn"),
            P("expert", "ffn", None),
            P("expert", None, None, ("dp", "ffn")),
            P("expert", ("dp", "ffn"), None),
            P("expert", None, "ffn"),
        ),
        check_vma=False,
    )
```
